32 devices in a mesh: dp: 1 (over z), tp: 4 (over y), sp: 8 (over x, core).
Axes of the slice: x: 4, y: 4, z: 1, core: 2. Of those that a mesh axis runs over, the one named last changes fastest.
The devices are a block of a 4x4x8 slice.
Arguments:
- hidden: bfloat16 [1024, 4096], P('dp')
- start_pos: int32 [1], P('dp')
- k_cache: bfloat16 [16384, 8, 128], P(('dp', 'sp'), 'tp')
- v_cache: bfloat16 [16384, 8, 128], P(('dp', 'sp'), 'tp')
- norm_gain: float32 [4096], replicated
- w_query: bfloat16 [4096, 4096], P(None, 'tp')
- w_key: bfloat16 [4096, 1024], P(None, 'tp')
- w_value: bfloat16 [4096, 1024], P(None, 'tp')
- q_gain: float32 [128], replicated
- k_gain: float32 [128], replicated
- w_out: bfloat16 [4096, 4096], P('tp')
Outputs:
- output 1: bfloat16 [1024, 4096], P('dp')
- output 2: bfloat16 [16384, 8, 128], P(('dp', 'sp'), 'tp')
- output 3: bfloat16 [16384, 8, 128], P(('dp', 'sp'), 'tp')
All inputs are finite; a program needn't handle non-finite values.
Results may differ from the reference program's by a relative error of at most 0.00426084.
Values sent between devices are 32-bit elements.
A program may use at most 768 MiB of HBM per device.

```python
import math
import jax
import jax.numpy as jnp
from jax import lax

MODEL_DIM = 4096
NUM_HEADS = 32
KV_HEADS = 8
HEAD_DIM = 128
CHUNK_LEN = 1024
CACHE_LEN = 16384
START_SLACK = 1024
GROUP_SIZE = NUM_HEADS // KV_HEADS
ROPE_BASE = 1e6
NORM_EPS = 1e-6
SCORE_SPREAD = math.sqrt(max(math.log(CACHE_LEN / 16.0), 1.0))
GAIN_CENTER = math.sqrt(SCORE_SPREAD)


def setup_inputs(seed: int = 0, part: int = 0) -> dict:
    base_key = jax.random.key(seed)
    part_keys = jax.random.split(jax.random.fold_in(base_key, part), 4)
    shared_keys = jax.random.split(base_key, 7)
    q_width = NUM_HEADS * HEAD_DIM
    kv_width = KV_HEADS * HEAD_DIM
    hidden = 0.5 * jax.random.normal(part_keys[0], (CHUNK_LEN, MODEL_DIM), jnp.float32)
    lowest = CACHE_LEN - CHUNK_LEN - START_SLACK
    start_pos = jax.random.randint(part_keys[1], (1,), lowest, lowest + START_SLACK + 1, jnp.int32)
    k_cache = GAIN_CENTER * jax.random.normal(part_keys[2], (CACHE_LEN, KV_HEADS, HEAD_DIM), jnp.float32)
    v_cache = jax.random.normal(part_keys[3], (CACHE_LEN, KV_HEADS, HEAD_DIM), jnp.float32)
    norm_gain = 1.0 + 0.3 * jax.random.normal(shared_keys[0], (MODEL_DIM,), jnp.float32)
    w_query = jax.random.normal(shared_keys[1], (MODEL_DIM, q_width), jnp.float32) * MODEL_DIM ** -0.5
    w_key = jax.random.normal(shared_keys[2], (MODEL_DIM, kv_width), jnp.float32) * MODEL_DIM ** -0.5
    w_value = jax.random.normal(shared_keys[3], (MODEL_DIM, kv_width), jnp.float32) * MODEL_DIM ** -0.5
    q_gain = GAIN_CENTER * (1.0 + 0.25 * jax.random.normal(shared_keys[4], (HEAD_DIM,), jnp.float32))
    k_gain = GAIN_CENTER * (1.0 + 0.25 * jax.random.normal(shared_keys[5], (HEAD_DIM,), jnp.float32))
    w_out = jax.random.normal(shared_keys[6], (q_width, MODEL_DIM), jnp.float32) * q_width ** -0.5
    return {
        "hidden": hidden.astype(jnp.bfloat16),
        "start_pos": start_pos,
        "k_cache": k_cache.astype(jnp.bfloat16),
        "v_cache": v_cache.astype(jnp.bfloat16),
        "norm_gain": norm_gain,
        "w_query": w_query.astype(jnp.bfloat16),
        "w_key": w_key.astype(jnp.bfloat16),
        "w_value": w_value.astype(jnp.bfloat16),
        "q_gain": q_gain,
        "k_gain": k_gain,
        "w_out": w_out.astype(jnp.bfloat16),
    }


def rms_norm(values, gain):
    mean_sq = jnp.mean(values * values, axis=-1, keepdims=True)
    return values * lax.rsqrt(mean_sq + NORM_EPS) * gain


def rotary(values, positions):
    half_dim = values.shape[-1] // 2
    inv_freq = ROPE_BASE ** (-2.0 * jnp.arange(half_dim, dtype=jnp.float32) / values.shape[-1])
    angles = positions.astype(jnp.float32)[:, None] * inv_freq[None, :]
    angles = angles.reshape((positions.shape[0],) + (1,) * (values.ndim - 2) + (half_dim,))
    cosine = jnp.cos(angles)
    sine = jnp.sin(angles)
    x_first = values[..., :half_dim]
    x_second = values[..., half_dim:]
    return jnp.concatenate([x_first * cosine - x_second * sine, x_second * cosine + x_first * sine], axis=-1)


def reference(hidden, start_pos, k_cache, v_cache, norm_gain, w_query, w_key, w_value, q_gain, k_gain, w_out):
    first_pos = start_pos[0]
    positions = first_pos + jnp.arange(CHUNK_LEN, dtype=jnp.int32)
    normed = rms_norm(hidden.astype(jnp.float32), norm_gain).astype(jnp.bfloat16)
    q_proj = jnp.dot(normed, w_query, preferred_element_type=jnp.float32).reshape(CHUNK_LEN, NUM_HEADS, HEAD_DIM)
    k_proj = jnp.dot(normed, w_key, preferred_element_type=jnp.float32).reshape(CHUNK_LEN, KV_HEADS, HEAD_DIM)
    v_proj = jnp.dot(normed, w_value, preferred_element_type=jnp.float32).reshape(CHUNK_LEN, KV_HEADS, HEAD_DIM)
    q_rot = rotary(rms_norm(q_proj, q_gain), positions).astype(jnp.bfloat16)
    k_rot = rotary(rms_norm(k_proj, k_gain), positions).astype(jnp.bfloat16)
    v_new = v_proj.astype(jnp.bfloat16)
    k_full = lax.dynamic_update_slice_in_dim(k_cache, k_rot, first_pos, axis=0)
    v_full = lax.dynamic_update_slice_in_dim(v_cache, v_new, first_pos, axis=0)
    key_pos = jnp.arange(CACHE_LEN, dtype=jnp.int32)
    allowed = key_pos[None, :] <= positions[:, None]
    att_scale = HEAD_DIM ** -0.5

    def one_head(head_index):
        kv_index = head_index // GROUP_SIZE
        q_head = lax.dynamic_index_in_dim(q_rot, head_index, axis=1, keepdims=False)
        k_head = lax.dynamic_index_in_dim(k_full, kv_index, axis=1, keepdims=False)
        v_head = lax.dynamic_index_in_dim(v_full, kv_index, axis=1, keepdims=False)
        scores = jnp.dot(q_head, k_head.T, preferred_element_type=jnp.float32) * att_scale
        scores = jnp.where(allowed, scores, -jnp.inf)
        row_max = jnp.max(scores, axis=-1, keepdims=True)
        weights = jnp.exp(scores - row_max)
        numerator = jnp.dot(weights.astype(jnp.bfloat16), v_head, preferred_element_type=jnp.float32)
        denominator = jnp.sum(weights, axis=-1, keepdims=True)
        return (numerator / denominator).astype(jnp.bfloat16)

    attention = lax.map(one_head, jnp.arange(NUM_HEADS, dtype=jnp.int32))
    attention_rows = jnp.transpose(attention, (1, 0, 2)).reshape(CHUNK_LEN, NUM_HEADS * HEAD_DIM)
    head_sum = jnp.dot(attention_rows, w_out, preferred_element_type=jnp.float32)
    out = (hidden.astype(jnp.float32) + head_sum).astype(jnp.bfloat16)
    return out, k_full, v_full
```

```python
import functools
import math

import jax
import jax.numpy as jnp
from jax import lax
from jax.experimental import pallas as pl
from jax.experimental.pallas import tpu as pltpu
from jax.sharding import PartitionSpec as P

ROPE_BASE = 1e6
NORM_EPS = 1e-6
LANES = 128
STAGES = 4
F32 = jnp.float32
BF16 = jnp.bfloat16
MESH = pl.DeviceIdType.MESH


def rms_norm(values, gain):
    mean_sq = jnp.mean(values * values, axis=-1, keepdims=True)
    return values * lax.rsqrt(mean_sq + NORM_EPS) * gain


def rope_tables(positions, head_dim):
    half_dim = head_dim // 2
    inv_freq = ROPE_BASE ** (-2.0 * jnp.arange(half_dim, dtype=F32) / head_dim)
    angles = positions.astype(F32)[:, None] * inv_freq[None, :]
    cosine, sine = jnp.cos(angles), jnp.sin(angles)
    return jnp.concatenate([cosine, cosine], axis=-1), jnp.concatenate([-sine, sine], axis=-1)


def rotate(values, cosine, sine):
    half = values.shape[-1] // 2
    return values * cosine + jnp.concatenate([values[..., half:], values[..., :half]], axis=-1) * sine


def attention_kernel(n_last, first_ref, h_ref, wq_ref, gain_ref, qg_ref, cos_ref, sin_ref, k_ref, v_ref, msg_ref, x_ref, q_ref):
    rows = h_ref.shape[0]
    kv_heads, shard_len, head_dim = k_ref.shape
    heads = wq_ref.shape[1] // head_dim
    group = heads // kv_heads
    step = pl.program_id(0)
    is_last = lax.axis_index("sp") == n_last
    scale = head_dim ** -0.5 * math.log2(math.e)

    hf = h_ref[...].astype(F32)
    mean_sq = jnp.mean(hf * hf, axis=-1, keepdims=True)
    x_ref[...] = (hf * lax.rsqrt(mean_sq + NORM_EPS) * gain_ref[...]).astype(BF16)
    cosine, sine = cos_ref[...], sin_ref[...]
    for pair in range(heads // 2):
        proj = jnp.dot(x_ref[...], wq_ref[:, pair * 2 * head_dim:(pair + 1) * 2 * head_dim], preferred_element_type=F32)
        for j in range(2):
            one = rms_norm(proj[:, j * head_dim:(j + 1) * head_dim], qg_ref[...])
            q_ref[pair * 2 + j] = (one * cosine + pltpu.roll(one, head_dim // 2, 1) * sine).astype(BF16)

    def attend(masked):
        lane = lax.broadcasted_iota(jnp.int32, (rows, LANES), 1)
        stats = jnp.zeros((rows, LANES), F32)
        if masked:
            key = lax.broadcasted_iota(jnp.int32, (rows, shard_len), 1)
            row = lax.broadcasted_iota(jnp.int32, (rows, shard_len), 0)
            allowed = key - row <= first_ref[0] + step * rows - n_last * shard_len
        for head in range(heads):
            kv = head // group
            s = lax.dot_general(q_ref[head], k_ref[kv], (((1,), (1,)), ((), ())), preferred_element_type=F32)
            if masked:
                s = jnp.where(allowed, s, -jnp.inf)
            m = jnp.max(s, axis=-1, keepdims=True)
            w = jnp.exp2((s - m) * scale)
            total = jnp.sum(w, axis=-1, keepdims=True)
            msg_ref[:, head * head_dim:(head + 1) * head_dim] = jnp.dot(w.astype(BF16), v_ref[kv], preferred_element_type=F32)
            stats = jnp.where(lane == head, m * scale, stats)
            stats = jnp.where(lane == heads + head, total, stats)
        msg_ref[:, heads * head_dim:] = stats

    @pl.when(is_last)
    def _():
        attend(True)

    @pl.when(jnp.logical_not(is_last))
    def _():
        attend(False)


def local_attention(n_last, first_pos, hidden, w_query, norm_gain, q_gain, cosine, sine, k_heads, v_heads):
    chunk, model = hidden.shape
    kv_heads, shard_len, head_dim = k_heads.shape
    width = w_query.shape[1]
    rows = chunk // STAGES
    once = pl.Buffered(buffer_count=1)
    whole = lambda *shape: pl.BlockSpec(shape, lambda i: (0,) * len(shape), pipeline_mode=once)
    return pl.pallas_call(
        functools.partial(attention_kernel, n_last),
        name="local_attention",
        grid=(STAGES,),
        out_shape=jax.ShapeDtypeStruct((chunk, width + LANES), F32),
        in_specs=[
            pl.BlockSpec(memory_space=pltpu.SMEM),
            pl.BlockSpec((rows, model), lambda i: (i, 0)),
            whole(model, width),
            whole(1, model),
            whole(1, head_dim),
            pl.BlockSpec((rows, head_dim), lambda i: (i, 0)),
            pl.BlockSpec((rows, head_dim), lambda i: (i, 0)),
            whole(kv_heads, shard_len, head_dim),
            whole(kv_heads, shard_len, head_dim),
        ],
        out_specs=pl.BlockSpec((rows, width + LANES), lambda i: (i, 0)),
        scratch_shapes=[pltpu.VMEM((rows, model), BF16), pltpu.VMEM((width // head_dim, rows, head_dim), BF16)],
        compiler_params=pltpu.CompilerParams(vmem_limit_bytes=60 * 2**20),
    )(first_pos, hidden, w_query, norm_gain.reshape(1, model), q_gain.reshape(1, head_dim), cosine, sine, k_heads, v_heads)


def merge(a, b, heads):
    d = (a.shape[1] - LANES) // heads
    sa, sb = a[:, heads * d:], b[:, heads * d:]
    top = jnp.maximum(sa, sb)
    ea, eb = jnp.exp2(sa - top), jnp.exp2(sb - top)
    lane = lax.broadcasted_iota(jnp.int32, sa.shape, 1)
    stats = jnp.where(lane < heads, top, sa * pltpu.roll(ea, heads, 1) + sb * pltpu.roll(eb, heads, 1))
    cols = [a[:, i * d:(i + 1) * d] * ea[:, i:i + 1] + b[:, i * d:(i + 1) * d] * eb[:, i:i + 1] for i in range(heads)]
    return jnp.concatenate(cols + [stats], axis=1)


def group_kernel(heads, nx, ny, msg_hbm, h_hbm, wout_hbm, out_hbm, msg, wout, chip, relay_x, final_x, part, relay_y, final_y, hrow, land, outb,
                 load_sem, send_sem, recv_sem, piece_sem, share_sem, share_send, out_sem):
    stages, srows, width = msg.shape
    model = wout.shape[1]
    half_model = model // 2
    plane = srows // 2
    xr_rows = plane // nx
    xh = xr_rows // 2
    yrows = xr_rows // ny
    sp = lax.axis_index("sp")
    y = lax.axis_index("tp")
    x, c = sp // 2, sp % 2
    oc = 1 - c
    x_r, x_l, x_o = (x + 1) % nx, (x + nx - 1) % nx, (x + 2) % nx
    y_r, y_l, y_o = (y + 1) % ny, (y + ny - 1) % ny, (y + 2) % ny
    partner = {"sp": x * 2 + oc}
    right, left = {"sp": x_r * 2 + c}, {"sp": x_l * 2 + c}
    up, down = {"tp": y_r}, {"tp": y_l}
    u = x * oc + y * c
    v = y * oc + x * c

    def axis_dev(d_first, d_second):
        return {"sp": ((x + oc * d_first + c * d_second + nx) % nx) * 2 + c, "tp": (y + c * d_first + oc * d_second + ny) % ny}

    u_r, u_l, v_r, v_l = axis_dev(1, 0), axis_dev(-1, 0), axis_dev(0, 1), axis_dev(0, -1)

    def piece_rows(du, dv):
        uu, vv = (u + du) % nx, (v + dv) % ny
        px, py = uu * oc + vv * c, vv * oc + uu * c
        return pl.multiple_of(c * plane + px * xr_rows + py * yrows, yrows)

    loads = [
        pltpu.make_async_copy(msg_hbm.at[pl.ds(b * srows, srows)], msg.at[b], load_sem.at[b]) for b in range(stages)
    ]
    for b in range(stages):
        loads[b].start()
    wout_load = pltpu.make_async_copy(wout_hbm, wout, load_sem.at[stages])
    wout_load.start()
    own_off = c * plane + x * xr_rows + y * yrows
    hloads = [
        pltpu.make_async_copy(h_hbm.at[pl.ds(pl.multiple_of(b * srows + own_off, yrows), yrows)], hrow.at[b], load_sem.at[stages + 1 + b])
        for b in range(stages)
    ]
    for b in range(stages):
        hloads[b].start()

    barrier = pltpu.get_barrier_semaphore()
    for dev in (partner, right, left, up, down):
        pl.semaphore_signal(barrier, inc=1, device_id=dev, device_id_type=MESH)
    pl.semaphore_wait(barrier, 5)

    def copy(src, dst, ssem, rsem, dev):
        return pltpu.make_async_remote_copy(src_ref=src, dst_ref=dst, send_sem=ssem, recv_sem=rsem, device_id=dev, device_id_type=MESH)

    def ds(start, size):
        return pl.ds(pl.multiple_of(start, size), size)

    def m_share(b):
        return copy(msg.at[b, ds(oc * plane, plane)], chip.at[b], send_sem.at[b, 0], recv_sem.at[b, 0], partner)

    def m_x(b, i):
        src, dst, dev = [
            (ds(x_o * xr_rows, xh), relay_x.at[b, 0], right),
            (ds(x_o * xr_rows + xh, xh), relay_x.at[b, 1], left),
            (ds(x_r * xr_rows + xh, xh), final_x.at[b, 0, pl.ds(xh, xh)], right),
            (ds(x_l * xr_rows, xh), final_x.at[b, 1, pl.ds(0, xh)], left),
            (ds(x_r * xr_rows, xh), final_x.at[b, 0, pl.ds(0, xh)], right),
            (ds(x_l * xr_rows + xh, xh), final_x.at[b, 1, pl.ds(xh, xh)], left),
        ][i]
        return copy(chip.at[b, src], dst, send_sem.at[b, 1 + i], recv_sem.at[b, 1 + i], dev)

    lo, hi = pl.ds(0, half_model), pl.ds(half_model, half_model)

    def m_y(b, i):
        src, dst, dev = [
            (part.at[b, ds(y_o * yrows, yrows), lo], relay_y.at[b, 0], up),
            (part.at[b, ds(y_o * yrows, yrows), hi], relay_y.at[b, 1], down),
            (part.at[b, ds(y_r * yrows, yrows), hi], final_y.at[b, 0, :, hi], up),
            (part.at[b, ds(y_l * yrows, yrows), lo], final_y.at[b, 1, :, lo], down),
            (part.at[b, ds(y_r * yrows, yrows), lo], final_y.at[b, 0, :, lo], up),
            (part.at[b, ds(y_l * yrows, yrows), hi], final_y.at[b, 1, :, hi], down),
        ][i]
        return copy(src, dst, send_sem.at[b, 7 + i], recv_sem.at[b, 7 + i], dev)

    def piece(b, du, dv, half):
        rows = pl.ds(piece_rows(du, dv), yrows)
        return land.at[b, rows] if half is None else land.at[b, rows, lo if half == 0 else hi]

    def sem_of(du, dv, half):
        return ((du % 4) * 4 + dv % 4) * 2 + (half or 0)

    def g_first(b, to, du, half):
        ref = piece(b, du, 0, half)
        s = sem_of(du - to, 0, half)
        return copy(ref, ref, send_sem.at[b, 13 + (0 if to == 1 else 1) + (2 if half is not None else 0)], piece_sem.at[b, s], u_r if to == 1 else u_l)

    def g_second(b, to, du, dv, half):
        ref = piece(b, du, dv, half)
        s = sem_of(du, dv - to, half)
        return copy(ref, ref, send_sem.at[b, 17 + (du % 4) * 4 + (0 if to == 1 else 1) + (2 if dv else 0)], piece_sem.at[b, s], v_r if to == 1 else v_l)

    def g_share(b, du, dv):
        ref = piece(b, du, dv, None)
        k = (du % 4) * 4 + dv % 4
        return copy(ref, ref, share_send.at[b, k], share_sem.at[b, k], partner)

    def wait_piece(b, du, dv, half):
        ref = piece(b, du, dv, half)
        copy(ref, ref, send_sem.at[b, 0], piece_sem.at[b, sem_of(du, dv, half)], partner).wait_recv()

    def wait_share(b, k):
        uu, vv = (x * c + y * oc + k // 4) % nx, (y * c + x * oc + k % 4) % nx
        row = oc * plane + (uu * c + vv * oc) * xr_rows + (vv * c + uu * oc) * yrows
        ref = land.at[b, pl.ds(pl.multiple_of(row, yrows), yrows)]
        copy(ref, ref, share_send.at[b, k], share_sem.at[b, k], partner).wait_recv()

    def s0(b):
        loads[b].wait()
        m_share(b).start()

    def s1(b):
        m_share(b).wait_recv()
        chip[b] = merge(chip[b], msg[b, ds(c * plane, plane)], heads)
        for i in range(4):
            m_x(b, i).start()

    def s2(b):
        for i, dest in ((0, x_r * xr_rows), (1, x_l * xr_rows + xh)):
            m_x(b, i).wait_recv()
            rows = ds(dest, xh)
            chip[b, rows] = merge(chip[b, rows], relay_x[b, i], heads)
            m_x(b, 4 + i).start()

    def s3(b):
        for i in range(2, 6):
            m_x(b, i).wait_recv()
        total = merge(chip[b, ds(x * xr_rows, xr_rows)], final_x[b, 0], heads)
        total = merge(total, final_x[b, 1], heads)
        d = (width - LANES) // heads
        base = heads * d + heads
        att = jnp.concatenate([(total[:, i * d:(i + 1) * d] / total[:, base + i:base + i + 1]).astype(BF16) for i in range(heads)], axis=1)
        for j in range(4):
            cols = slice(j * (model // 4), (j + 1) * (model // 4))
            part[b, :, cols] = jnp.dot(att, wout[:, cols], preferred_element_type=F32)
        for i in range(4):
            m_y(b, i).start()

    def s4(b):
        for i, (dest, cols) in enumerate(((y_r, lo), (y_l, hi))):
            m_y(b, i).wait_recv()
            rows = ds(dest * yrows, yrows)
            part[b, rows, cols] = part[b, rows, cols] + relay_y[b, i]
            m_y(b, 4 + i).start()

    def s5(b):
        for i in range(2, 6):
            m_y(b, i).wait_recv()
        total = part[b, ds(y * yrows, yrows)] + final_y[b, 0] + final_y[b, 1]
        land[b, pl.ds(piece_rows(0, 0), yrows)] = total + hrow[b].astype(F32)
        g_first(b, 1, 0, None).start()
        g_first(b, -1, 0, None).start()
        g_second(b, 1, 0, 0, None).start()
        g_second(b, -1, 0, 0, None).start()
        g_share(b, 0, 0).start()

    def arrive_second(b, du):
        wait_piece(b, du, -1, None)
        g_second(b, 1, du, -1, 0).start()
        wait_piece(b, du, 1, None)
        g_second(b, -1, du, 1, 1).start()
        g_share(b, du, -1).start()
        g_share(b, du, 1).start()

    def arrive_far(b, du):
        for half in range(2):
            wait_piece(b, du, 2, half)
        g_share(b, du, 2).start()

    def s6(b):
        wait_piece(b, -1, 0, None)
        g_first(b, 1, -1, 0).start()
        wait_piece(b, 1, 0, None)
        g_first(b, -1, 1, 1).start()
        for du in (-1, 1):
            g_second(b, 1, du, 0, None).start()
            g_second(b, -1, du, 0, None).start()
            g_share(b, du, 0).start()
        arrive_second(b, 0)

    def s7(b):
        wait_piece(b, 2, 0, 0)
        wait_piece(b, 2, 0, 1)
        g_second(b, 1, 2, 0, None).start()
        g_second(b, -1, 2, 0, None).start()
        g_share(b, 2, 0).start()
        arrive_second(b, -1)
        arrive_second(b, 1)
        arrive_far(b, 0)

    def s8(b):
        arrive_second(b, 2)
        arrive_far(b, -1)
        arrive_far(b, 1)

    def s9(b):
        arrive_far(b, 2)

    def out_copy(b):
        return pltpu.make_async_copy(outb.at[b], out_hbm.at[pl.ds(pl.multiple_of(b * srows, srows), srows)], out_sem.at[b])

    def s10(b):
        for k in range(16):
            wait_share(b, k)
        @pl.loop(0, srows // 16)
        def _(r):
            rows = pl.ds(pl.multiple_of(r * 16, 16), 16)
            outb[b, rows] = land[b, rows].astype(BF16)
        out_copy(b).start()

    steps = [s0, s1, s2, s3, s4, s5, s6, s7, s8, s9, s10]
    wout_load.wait()
    for b in range(stages):
        hloads[b].wait()
    gap = 1
    for t in range((stages - 1) * gap + len(steps)):
        for k in reversed(range(len(steps))):
            if (t - k) % gap == 0 and 0 <= (t - k) // gap < stages:
                steps[k]((t - k) // gap)
    for b in range(stages):
        m_share(b).wait_send()
        for i in range(6):
            m_x(b, i).wait_send()
            m_y(b, i).wait_send()
        for to in (1, -1):
            g_first(b, to, 0, None).wait_send()
            g_first(b, to, -to, 0 if to == 1 else 1).wait_send()
            for du in range(4):
                g_second(b, to, du, 0, None).wait_send()
                g_second(b, to, du, -to, 0 if to == 1 else 1).wait_send()
        for du in range(4):
            for dv in range(4):
                g_share(b, du, dv).wait_send()
        out_copy(b).wait()


def combine(mesh, msg, hidden, w_out, heads):
    chunk, model = hidden.shape
    width = msg.shape[1]
    nx, ny = mesh.shape["sp"] // 2, mesh.shape["tp"]
    assert nx == 4 and ny == 4
    srows = chunk // STAGES
    plane = srows // 2
    xr_rows = plane // nx
    yrows = xr_rows // ny
    dma = pltpu.SemaphoreType.DMA
    return pl.pallas_call(
        functools.partial(group_kernel, heads, nx, ny),
        name="group_combine",
        out_shape=jax.ShapeDtypeStruct((chunk, model), BF16),
        in_specs=[pl.BlockSpec(memory_space=pl.ANY)] * 3,
        out_specs=pl.BlockSpec(memory_space=pl.ANY),
        scratch_shapes=[
            pltpu.VMEM((STAGES, srows, width), F32),
            pltpu.VMEM(w_out.shape, BF16),
            pltpu.VMEM((STAGES, plane, width), F32),
            pltpu.VMEM((STAGES, 2, xr_rows // 2, width), F32),
            pltpu.VMEM((STAGES, 2, xr_rows, width), F32),
            pltpu.VMEM((STAGES, xr_rows, model), F32),
            pltpu.VMEM((STAGES, 2, yrows, model // 2), F32),
            pltpu.VMEM((STAGES, 2, yrows, model), F32),
            pltpu.VMEM((STAGES, yrows, model), BF16),
            pltpu.VMEM((STAGES, srows, model), F32),
            pltpu.VMEM((STAGES, srows, model), BF16),
            dma((2 * STAGES + 1,)),
            dma((STAGES, 33)),
            dma((STAGES, 13)),
            dma((STAGES, 32)),
            dma((STAGES, 16)),
            dma((STAGES, 16)),
            dma((STAGES,)),
        ],
        compiler_params=pltpu.CompilerParams(collective_id=0, has_side_effects=True, vmem_limit_bytes=63 * 2**20),
    )(msg, hidden, w_out)


def solution(mesh):
    cache_spec = P(("dp", "sp"), "tp", None)
    in_specs = (P("dp", None), P("dp"), cache_spec, cache_spec, P(None), P(None, "tp"), P(None, "tp"), P(None, "tp"), P(None), P(None), P("tp", None))
    out_specs = (P("dp", None), cache_spec, cache_spec)
    n_last = mesh.shape["sp"] - 1

    def local_step(hidden, start_pos, k_shard, v_shard, norm_gain, w_query, w_key, w_value, q_gain, k_gain, w_out):
        chunk_len, model_dim = hidden.shape
        shard_len, kv_local, head_dim = k_shard.shape
        heads = w_query.shape[1] // head_dim
        first_pos = start_pos[0]
        cosine, sine = rope_tables(first_pos + jnp.arange(chunk_len, dtype=jnp.int32), head_dim)

        def with_new(k_old, v_old):
            write_at = first_pos - n_last * shard_len
            normed = rms_norm(hidden.astype(F32), norm_gain).astype(BF16)
            k_proj = jnp.dot(normed, w_key, preferred_element_type=F32).reshape(chunk_len, kv_local, head_dim)
            v_new = jnp.dot(normed, w_value, preferred_element_type=F32).reshape(chunk_len, kv_local, head_dim).astype(BF16)
            k_rot = rotate(rms_norm(k_proj, k_gain), cosine[:, None, :], sine[:, None, :]).astype(BF16)
            return (lax.dynamic_update_slice(k_old, k_rot, (write_at, 0, 0)), lax.dynamic_update_slice(v_old, v_new, (write_at, 0, 0)))

        k_upd, v_upd = lax.cond(lax.axis_index("sp") == n_last, with_new, lambda k_old, v_old: (k_old, v_old), k_shard, v_shard)
        k_heads, v_heads = jnp.transpose(k_upd, (1, 0, 2)), jnp.transpose(v_upd, (1, 0, 2))
        msg = local_attention(n_last, start_pos, hidden, w_query, norm_gain, q_gain, cosine, sine, k_heads, v_heads)
        out = combine(mesh, msg, hidden, w_out, heads)
        return out, k_upd, v_upd

    return jax.shard_map(local_step, mesh=mesh, in_specs=in_specs, out_specs=out_specs, check_vma=False)
```

```python
import functools
import math

import jax
import jax.numpy as jnp
from jax import lax
from jax.experimental import pallas as pl
from jax.experimental.pallas import tpu as pltpu
from jax.sharding import PartitionSpec as P

ROPE_BASE = 1e6
NORM_EPS = 1e-6
LANES = 128
STAGES = 4
STEP_AT = (
    (5, 10, 15, 20), (6, 11, 16, 21), (8, 13, 18, 22), (10, 15, 20, 24), (11, 16, 22, 27), (12, 18, 23, 28),
    (14, 20, 25, 29), (16, 22, 28, 31), (18, 24, 29, 32), (19, 26, 30, 33), (20, 27, 31, 34),
)
F32 = jnp.float32
BF16 = jnp.bfloat16
MESH = pl.DeviceIdType.MESH


def rms_norm(values, gain):
    mean_sq = jnp.mean(values * values, axis=-1, keepdims=True)
    return values * lax.rsqrt(mean_sq + NORM_EPS) * gain


def rope_tables(positions, head_dim):
    half_dim = head_dim // 2
    inv_freq = ROPE_BASE ** (-2.0 * jnp.arange(half_dim, dtype=F32) / head_dim)
    angles = positions.astype(F32)[:, None] * inv_freq[None, :]
    cosine, sine = jnp.cos(angles), jnp.sin(angles)
    return jnp.concatenate([cosine, cosine], axis=-1), jnp.concatenate([-sine, sine], axis=-1)


def merge(a, b, heads):
    d = (a.shape[1] - LANES) // heads
    sa, sb = a[:, heads * d:], b[:, heads * d:]
    top = jnp.maximum(sa, sb)
    ea, eb = jnp.exp2(sa - top), jnp.exp2(sb - top)
    lane = lax.broadcasted_iota(jnp.int32, sa.shape, 1)
    stats = jnp.where(lane < heads, top, sa * pltpu.roll(ea, heads, 1) + sb * pltpu.roll(eb, heads, 1))
    cols = [a[:, i * d:(i + 1) * d] * ea[:, i:i + 1] + b[:, i * d:(i + 1) * d] * eb[:, i:i + 1] for i in range(heads)]
    return jnp.concatenate(cols + [stats], axis=1)


def group_kernel(n_last, nx, ny, at_ref, h_hbm, wq_hbm, wk_hbm, wv_hbm, gain_ref, qg_ref, kg_ref, cos_hbm, sin_hbm, k_hbm, v_hbm, wout_hbm,
                 out_hbm, kn_hbm, vn_hbm,
                 wq, wk, wv, wout, h_buf, x_buf, cos_buf, sin_buf, k_buf, v_buf, q_buf, s0_buf, s1_buf, p0_buf, p1_buf, bias_old, bias_new, new_f32, k_rows, v_rows,
                 msg, chip, relay_x, final_x, part, relay_y, final_y, hrow, land, outb,
                 load_sem, table_sem, h_sem, hrow_sem, rows_sem, send_sem, recv_sem, piece_sem, share_sem, share_send, out_sem):
    stages, plane, width = chip.shape
    srows = 2 * plane
    model = wout.shape[1]
    half_model = model // 2
    xr_rows = plane // nx
    xh = xr_rows // 2
    yrows = xr_rows // ny
    sp = lax.axis_index("sp")
    y = lax.axis_index("tp")
    x, c = sp // 2, sp % 2
    oc = 1 - c
    x_r, x_l, x_o = (x + 1) % nx, (x + nx - 1) % nx, (x + 2) % nx
    y_r, y_l, y_o = (y + 1) % ny, (y + ny - 1) % ny, (y + 2) % ny
    partner = {"sp": x * 2 + oc}
    right, left = {"sp": x_r * 2 + c}, {"sp": x_l * 2 + c}
    up, down = {"tp": y_r}, {"tp": y_l}
    u = x * oc + y * c
    v = y * oc + x * c

    def axis_dev(d_first, d_second):
        return {"sp": ((x + oc * d_first + c * d_second + nx) % nx) * 2 + c, "tp": (y + c * d_first + oc * d_second + ny) % ny}

    u_r, u_l, v_r, v_l = axis_dev(1, 0), axis_dev(-1, 0), axis_dev(0, 1), axis_dev(0, -1)

    def piece_rows(du, dv):
        uu, vv = (u + du) % nx, (v + dv) % ny
        px, py = uu * oc + vv * c, vv * oc + uu * c
        return pl.multiple_of(c * plane + px * xr_rows + py * yrows, yrows)

    kv_heads, shard_len, head_dim = k_buf.shape
    heads = wq.shape[1] // head_dim
    group = heads // kv_heads
    old = shard_len - stages * srows
    pairs = heads // 2
    parts = 1 + pairs
    is_last = sp == n_last
    scale = head_dim ** -0.5 * math.log2(math.e)

    def ds(start, size):
        return pl.ds(pl.multiple_of(start, size), size)

    def h_load(b):
        return pltpu.make_async_copy(h_hbm.at[ds(b * srows, srows)], h_buf, h_sem.at[b])

    own_off = c * plane + x * xr_rows + y * yrows

    def hrow_load(b):
        return pltpu.make_async_copy(h_hbm.at[ds(b * srows + own_off, yrows)], hrow.at[b], hrow_sem.at[b])

    loads = [
        pltpu.make_async_copy(src, dst, load_sem.at[i])
        for i, (src, dst) in enumerate(((wq_hbm, wq), (k_hbm, k_buf), (v_hbm, v_buf), (wout_hbm, wout), (wk_hbm, wk), (wv_hbm, wv)))
    ]

    def table_load(b, i):
        src, dst = ((cos_hbm, cos_buf), (sin_hbm, sin_buf))[i]
        return pltpu.make_async_copy(src.at[ds(b * srows, srows)], dst.at[b % 2], table_sem.at[b, i])

    h_load(0).start()
    for i in range(2):
        table_load(0, i).start()
    for i in range(3):
        loads[i].start()

    @pl.when(is_last)
    def _():
        loads[4].start()
        loads[5].start()

    loads[3].start()
    for b in range(stages):
        hrow_load(b).start()

    barrier = pltpu.get_barrier_semaphore()
    for dev in (partner, right, left, up, down):
        pl.semaphore_signal(barrier, inc=1, device_id=dev, device_id_type=MESH)
    pl.semaphore_wait(barrier, 5)

    def copy(src, dst, ssem, rsem, dev):
        return pltpu.make_async_remote_copy(src_ref=src, dst_ref=dst, send_sem=ssem, recv_sem=rsem, device_id=dev, device_id_type=MESH)

    def m_share(b):
        return copy(msg.at[b % 2, ds(oc * plane, plane)], chip.at[b], send_sem.at[b, 0], recv_sem.at[b, 0], partner)

    def m_x(b, i):
        src, dst, dev = [
            (ds(x_o * xr_rows, xh), relay_x.at[b, 0], right),
            (ds(x_o * xr_rows + xh, xh), relay_x.at[b, 1], left),
            (ds(x_r * xr_rows + xh, xh), final_x.at[b, 0, pl.ds(xh, xh)], right),
            (ds(x_l * xr_rows, xh), final_x.at[b, 1, pl.ds(0, xh)], left),
            (ds(x_r * xr_rows, xh), final_x.at[b, 0, pl.ds(0, xh)], right),
            (ds(x_l * xr_rows + xh, xh), final_x.at[b, 1, pl.ds(xh, xh)], left),
        ][i]
        return copy(chip.at[b, src], dst, send_sem.at[b, 1 + i], recv_sem.at[b, 1 + i], dev)

    lo, hi = pl.ds(0, half_model), pl.ds(half_model, half_model)

    def m_y(b, i):
        src, dst, dev = [
            (part.at[b, ds(y_o * yrows, yrows), lo], relay_y.at[b, 0], up),
            (part.at[b, ds(y_o * yrows, yrows), hi], relay_y.at[b, 1], down),
            (part.at[b, ds(y_r * yrows, yrows), hi], final_y.at[b, 0, :, hi], up),
            (part.at[b, ds(y_l * yrows, yrows), lo], final_y.at[b, 1, :, lo], down),
            (part.at[b, ds(y_r * yrows, yrows), lo], final_y.at[b, 0, :, lo], up),
            (part.at[b, ds(y_l * yrows, yrows), hi], final_y.at[b, 1, :, hi], down),
        ][i]
        return copy(src, dst, send_sem.at[b, 7 + i], recv_sem.at[b, 7 + i], dev)

    def piece(b, du, dv, half):
        rows = pl.ds(piece_rows(du, dv), yrows)
        return land.at[b, rows] if half is None else land.at[b, rows, lo if half == 0 else hi]

    def sem_of(du, dv, half):
        return ((du % 4) * 4 + dv % 4) * 2 + (half or 0)

    def g_first(b, to, du, half):
        ref = piece(b, du, 0, half)
        s = sem_of(du - to, 0, half)
        return copy(ref, ref, send_sem.at[b, 13 + (0 if to == 1 else 1) + (2 if half is not None else 0)], piece_sem.at[b, s], u_r if to == 1 else u_l)

    def g_second(b, to, du, dv, half):
        ref = piece(b, du, dv, half)
        s = sem_of(du, dv - to, half)
        return copy(ref, ref, send_sem.at[b, 17 + (du % 4) * 4 + (0 if to == 1 else 1) + (2 if dv else 0)], piece_sem.at[b, s], v_r if to == 1 else v_l)

    def g_share(b, du, dv):
        ref = piece(b, du, dv, None)
        k = (du % 4) * 4 + dv % 4
        return copy(ref, ref, share_send.at[b, k], share_sem.at[b, k], partner)

    def wait_piece(b, du, dv, half):
        ref = piece(b, du, dv, half)
        copy(ref, ref, send_sem.at[b, 0], piece_sem.at[b, sem_of(du, dv, half)], partner).wait_recv()

    def wait_share(b, k):
        uu, vv = (x * c + y * oc + k // 4) % nx, (y * c + x * oc + k % 4) % nx
        row = oc * plane + (uu * c + vv * oc) * xr_rows + (vv * c + uu * oc) * yrows
        ref = land.at[b, pl.ds(pl.multiple_of(row, yrows), yrows)]
        copy(ref, ref, share_send.at[b, k], share_sem.at[b, k], partner).wait_recv()

    def s0(b):
        m_share(b).start()

    def s1(b):
        m_share(b).wait_recv()
        chip[b] = merge(chip[b], msg[b % 2, ds(c * plane, plane)], heads)
        for i in range(4):
            m_x(b, i).start()

    def s2(b):
        for i, dest in ((0, x_r * xr_rows), (1, x_l * xr_rows + xh)):
            m_x(b, i).wait_recv()
            rows = ds(dest, xh)
            chip[b, rows] = merge(chip[b, rows], relay_x[b, i], heads)
            m_x(b, 4 + i).start()

    def s3(b):
        @pl.when(b == 0)
        def _():
            loads[3].wait()

        for i in range(2, 6):
            m_x(b, i).wait_recv()
        total = merge(chip[b, ds(x * xr_rows, xr_rows)], final_x[b, 0], heads)
        total = merge(total, final_x[b, 1], heads)
        d = (width - LANES) // heads
        base = heads * d + heads
        att = jnp.concatenate([(total[:, i * d:(i + 1) * d] / total[:, base + i:base + i + 1]).astype(BF16) for i in range(heads)], axis=1)
        for j in range(4):
            cols = slice(j * (model // 4), (j + 1) * (model // 4))
            part[b, :, cols] = jnp.dot(att, wout[:, cols], preferred_element_type=F32)
        for i in range(4):
            m_y(b, i).start()

    def s4(b):
        for i, (dest, cols) in enumerate(((y_r, lo), (y_l, hi))):
            m_y(b, i).wait_recv()
            rows = ds(dest * yrows, yrows)
            part[b, rows, cols] = part[b, rows, cols] + relay_y[b, i]
            m_y(b, 4 + i).start()

    def s5(b):
        for i in range(2, 6):
            m_y(b, i).wait_recv()
        hrow_load(b).wait()
        total = part[b, ds(y * yrows, yrows)] + final_y[b, 0] + final_y[b, 1]
        land[b, pl.ds(piece_rows(0, 0), yrows)] = total + hrow[b].astype(F32)
        g_first(b, 1, 0, None).start()
        g_first(b, -1, 0, None).start()
        g_second(b, 1, 0, 0, None).start()
        g_second(b, -1, 0, 0, None).start()
        g_share(b, 0, 0).start()

    def arrive_second(b, du):
        wait_piece(b, du, -1, None)
        g_second(b, 1, du, -1, 0).start()
        wait_piece(b, du, 1, None)
        g_second(b, -1, du, 1, 1).start()
        g_share(b, du, -1).start()
        g_share(b, du, 1).start()

    def arrive_far(b, du):
        for half in range(2):
            wait_piece(b, du, 2, half)
        g_share(b, du, 2).start()

    def s6(b):
        wait_piece(b, -1, 0, None)
        g_first(b, 1, -1, 0).start()
        wait_piece(b, 1, 0, None)
        g_first(b, -1, 1, 1).start()
        for du in (-1, 1):
            g_second(b, 1, du, 0, None).start()
            g_second(b, -1, du, 0, None).start()
            g_share(b, du, 0).start()
        arrive_second(b, 0)

    def s7(b):
        wait_piece(b, 2, 0, 0)
        wait_piece(b, 2, 0, 1)
        g_second(b, 1, 2, 0, None).start()
        g_second(b, -1, 2, 0, None).start()
        g_share(b, 2, 0).start()
        arrive_second(b, -1)
        arrive_second(b, 1)
        arrive_far(b, 0)

    def s8(b):
        arrive_second(b, 2)
        arrive_far(b, -1)
        arrive_far(b, 1)

    def s9(b):
        arrive_far(b, 2)

    def out_copy(b):
        return pltpu.make_async_copy(outb, out_hbm.at[pl.ds(pl.multiple_of(b * srows, srows), srows)], out_sem.at[b])

    def s10(b):
        for k in range(16):
            wait_share(b, k)

        @pl.when(b > 0)
        def _():
            out_copy(b - 1).wait()

        @pl.loop(0, srows // 16)
        def _(r):
            rows = pl.ds(pl.multiple_of(r * 16, 16), 16)
            outb[rows] = land[b, rows].astype(BF16)
        out_copy(b).start()

    lane = lax.broadcasted_iota(jnp.int32, (srows, LANES), 1)
    s_bufs, p_bufs = (s0_buf, s1_buf), (p0_buf, p1_buf)

    def kv_rows_copy(b, i):
        src, dst = ((k_rows, kn_hbm), (v_rows, vn_hbm))[i]
        return pltpu.make_async_copy(src, dst.at[ds(b * srows, srows)], rows_sem.at[b, i])

    def scores(head, slot, kb):
        q, k = q_buf[head], head // group
        nt = (((1,), (1,)), ((), ()))
        if kb is None:
            s_bufs[slot][...] = lax.dot_general(q, k_buf[k], nt, preferred_element_type=F32)
            return
        seen = old + kb * srows
        s_bufs[slot][:, :old] = lax.dot_general(q, k_buf[k, :old], nt, preferred_element_type=F32) + bias_old[...]
        if kb:
            s_bufs[slot][:, old:seen] = lax.dot_general(q, k_buf[k, old:seen], nt, preferred_element_type=F32)
        s_bufs[slot][:, seen:seen + srows] = lax.dot_general(q, k_buf[k, seen:seen + srows], nt, preferred_element_type=F32) + bias_new[...]

    def one_head(b, head, slot, kb, stats):
        keys = shard_len if kb is None else old + (kb + 1) * srows
        s = s_bufs[slot][:, :keys]
        m = jnp.max(s, axis=-1, keepdims=True)
        w = jnp.exp2((s - m) * scale)
        total = jnp.sum(w, axis=-1, keepdims=True)
        p_bufs[slot][:, :keys] = w.astype(BF16)
        num = jnp.dot(p_bufs[slot][:, :keys], v_buf[head // group, :keys], preferred_element_type=F32)
        msg[b % 2, :, pl.ds(pl.multiple_of(head * head_dim, head_dim), head_dim)] = num
        return jnp.where(lane == head, m * scale, jnp.where(lane == heads + head, total, stats))

    def each_variant(b, fn):
        @pl.when(jnp.logical_not(is_last))
        def _():
            fn(None)

        for kb in range(stages):
            @pl.when(jnp.logical_and(is_last, b == kb))
            def _():
                fn(kb)

    def project(b):
        @pl.when(b >= 2)
        def _():
            m_share(b - 2).wait_send()

        h_load(b).wait()

        @pl.loop(0, srows // 16, unroll=2)
        def _(r):
            rows = ds(r * 16, 16)
            hf = h_buf[rows].astype(F32)
            mean_sq = jnp.mean(hf * hf, axis=-1, keepdims=True)
            x_buf[rows] = (hf * lax.rsqrt(mean_sq + NORM_EPS) * gain_ref[...]).astype(BF16)

        @pl.when(b + 1 < stages)
        def _():
            h_load(b + 1).start()
            table_load(b + 1, 0).start()
            table_load(b + 1, 1).start()

        @pl.when(b == 0)
        def _():
            for i in range(3):
                loads[i].wait()

        table_load(b, 0).wait()
        table_load(b, 1).wait()

        def rope(one):
            return one * cos_buf[b % 2] + pltpu.roll(one, head_dim // 2, 1) * sin_buf[b % 2]

        def project_pair(pair, carry):
            proj = jnp.dot(x_buf[...], wq[:, ds(pair * 2 * head_dim, 2 * head_dim)], preferred_element_type=F32)
            for j in range(2):
                q_buf[pair * 2 + j] = rope(rms_norm(proj[:, j * head_dim:(j + 1) * head_dim], qg_ref[...])).astype(BF16)
            return carry

        lax.fori_loop(0, pairs, project_pair, 0)

        @pl.when(is_last)
        def _():
            @pl.when(b == 0)
            def _():
                loads[4].wait()
                loads[5].wait()
                key = lax.broadcasted_iota(jnp.int32, bias_old.shape, 1)
                bias_old[...] = jnp.where(key < at_ref[0], 0.0, -jnp.inf)
                row = lax.broadcasted_iota(jnp.int32, bias_new.shape, 0)
                col = lax.broadcasted_iota(jnp.int32, bias_new.shape, 1)
                bias_new[...] = jnp.where(col <= row, 0.0, -jnp.inf)

            @pl.when(b > 0)
            def _():
                kv_rows_copy(b - 1, 0).wait()
                kv_rows_copy(b - 1, 1).wait()

            new = ds(old + b * srows, srows)
            proj = jnp.dot(x_buf[...], wk[...], preferred_element_type=F32)
            for j in range(kv_heads):
                one = rope(rms_norm(proj[:, j * head_dim:(j + 1) * head_dim], kg_ref[...]))
                k_buf[j, new] = one.astype(BF16)
                new_f32[:, j, :] = one
            k_rows[...] = new_f32[...].astype(BF16)
            proj = jnp.dot(x_buf[...], wv[...], preferred_element_type=F32)
            for j in range(kv_heads):
                one = proj[:, j * head_dim:(j + 1) * head_dim]
                v_buf[j, new] = one.astype(BF16)
                new_f32[:, j, :] = one
            v_rows[...] = new_f32[...].astype(BF16)
            kv_rows_copy(b, 0).start()
            kv_rows_copy(b, 1).start()

        msg[b % 2, :, heads * head_dim:] = jnp.zeros((srows, LANES), F32)
        each_variant(b, lambda kb: scores(0, 0, kb))

    def attend_pair(b, j):
        def run(kb):
            stats = msg[b % 2, :, heads * head_dim:]
            scores(2 * j + 1, 1, kb)
            stats = one_head(b, 2 * j, 0, kb, stats)
            scores(jnp.minimum(2 * j + 2, heads - 1), 0, kb)
            msg[b % 2, :, heads * head_dim:] = one_head(b, 2 * j + 1, 1, kb, stats)

        each_variant(b, run)

    steps = [s0, s1, s2, s3, s4, s5, s6, s7, s8, s9, s10]

    @pl.loop(0, max(STEP_AT[-1]) + 1)
    def _(t):
        for k in reversed(range(len(steps))):
            due, passed = t == STEP_AT[k][0], 0
            for at in STEP_AT[k][1:]:
                due = jnp.logical_or(due, t == at)
                passed = passed + (t >= at).astype(jnp.int32)

            @pl.when(due)
            def _():
                steps[k](passed)

        b = t // parts

        @pl.when(jnp.logical_and(b < stages, t % parts == 0))
        def _():
            project(b)

        @pl.when(jnp.logical_and(b < stages, t % parts > 0))
        def _():
            attend_pair(b, t % parts - 1)

    @pl.when(is_last)
    def _():
        kv_rows_copy(stages - 1, 0).wait()
        kv_rows_copy(stages - 1, 1).wait()

    out_copy(stages - 1).wait()
    for b in range(stages):
        if b >= stages - 2:
            m_share(b).wait_send()
        for i in range(6):
            m_x(b, i).wait_send()
            m_y(b, i).wait_send()
        for to in (1, -1):
            g_first(b, to, 0, None).wait_send()
            g_first(b, to, -to, 0 if to == 1 else 1).wait_send()
            for du in range(4):
                g_second(b, to, du, 0, None).wait_send()
                g_second(b, to, du, -to, 0 if to == 1 else 1).wait_send()
        for du in range(4):
            for dv in range(4):
                g_share(b, du, dv).wait_send()


def attend_and_combine(mesh, write_at, hidden, w_query, w_key, w_value, norm_gain, q_gain, k_gain, cosine, sine, k_heads, v_heads, w_out):
    chunk, model = hidden.shape
    kv_heads, shard_len, head_dim = k_heads.shape
    width = w_query.shape[1] + LANES
    kv_width = w_key.shape[1]
    nx, ny = mesh.shape["sp"] // 2, mesh.shape["tp"]
    assert nx == 4 and ny == 4
    srows = chunk // STAGES
    plane = srows // 2
    xr_rows = plane // nx
    yrows = xr_rows // ny
    dma = pltpu.SemaphoreType.DMA
    anywhere = pl.BlockSpec(memory_space=pl.ANY)
    vmem = pl.BlockSpec(memory_space=pltpu.VMEM)
    new_rows = jax.ShapeDtypeStruct((chunk, kv_heads, head_dim), BF16)
    return pl.pallas_call(
        functools.partial(group_kernel, mesh.shape["sp"] - 1, nx, ny),
        name="attend_and_combine",
        out_shape=(jax.ShapeDtypeStruct((chunk, model), BF16), new_rows, new_rows),
        in_specs=[pl.BlockSpec(memory_space=pltpu.SMEM)] + [anywhere] * 4 + [vmem] * 3 + [anywhere] * 5,
        out_specs=(anywhere,) * 3,
        scratch_shapes=[
            pltpu.VMEM(w_query.shape, BF16),
            pltpu.VMEM(w_key.shape, BF16),
            pltpu.VMEM(w_value.shape, BF16),
            pltpu.VMEM(w_out.shape, BF16),
            pltpu.VMEM((srows, model), BF16),
            pltpu.VMEM((srows, model), BF16),
            pltpu.VMEM((2, srows, head_dim), F32),
            pltpu.VMEM((2, srows, head_dim), F32),
            pltpu.VMEM(k_heads.shape, BF16),
            pltpu.VMEM(v_heads.shape, BF16),
            pltpu.VMEM((w_query.shape[1] // head_dim, srows, head_dim), BF16),
            pltpu.VMEM((srows, shard_len), F32),
            pltpu.VMEM((srows, shard_len), F32),
            pltpu.VMEM((srows, shard_len), BF16),
            pltpu.VMEM((srows, shard_len), BF16),
            pltpu.VMEM((1, shard_len - chunk), F32),
            pltpu.VMEM((srows, srows), F32),
            pltpu.VMEM((srows, kv_heads, head_dim), F32),
            pltpu.VMEM((srows, kv_heads, head_dim), BF16),
            pltpu.VMEM((srows, kv_heads, head_dim), BF16),
            pltpu.VMEM((2, srows, width), F32),
            pltpu.VMEM((STAGES, plane, width), F32),
            pltpu.VMEM((STAGES, 2, xr_rows // 2, width), F32),
            pltpu.VMEM((STAGES, 2, xr_rows, width), F32),
            pltpu.VMEM((STAGES, xr_rows, model), F32),
            pltpu.VMEM((STAGES, 2, yrows, model // 2), F32),
            pltpu.VMEM((STAGES, 2, yrows, model), F32),
            pltpu.VMEM((STAGES, yrows, model), BF16),
            pltpu.VMEM((STAGES, srows, model), F32),
            pltpu.VMEM((srows, model), BF16),
            dma((6,)),
            dma((STAGES, 2)),
            dma((STAGES,)),
            dma((STAGES,)),
            dma((STAGES, 2)),
            dma((STAGES, 33)),
            dma((STAGES, 13)),
            dma((STAGES, 32)),
            dma((STAGES, 16)),
            dma((STAGES, 16)),
            dma((STAGES,)),
        ],
        compiler_params=pltpu.CompilerParams(collective_id=0, has_side_effects=True, vmem_limit_bytes=67043328),
    )(write_at.reshape(1), hidden, w_query, w_key, w_value, norm_gain.reshape(1, model), q_gain.reshape(1, head_dim), k_gain.reshape(1, head_dim),
      cosine, sine, k_heads, v_heads, w_out)


def finish_kernel(n_last, pieces, at_ref, out_in, k_in, v_in, kn_in, vn_in, out_ref, k_out, v_out, out_buf, k_buf, v_buf, kn_buf, vn_buf, sem):
    is_last = lax.axis_index("sp") == n_last
    rows = out_in.shape[0] // pieces
    reads = [pltpu.make_async_copy(k_in, k_buf, sem.at[0, 0]), pltpu.make_async_copy(v_in, v_buf, sem.at[0, 1])]
    writes = [pltpu.make_async_copy(k_buf, k_out, sem.at[1, 0]), pltpu.make_async_copy(v_buf, v_out, sem.at[1, 1])]
    for i in range(pieces):
        here = pl.ds(i * rows, rows)
        reads.append(pltpu.make_async_copy(out_in.at[here], out_buf.at[here], sem.at[0, 2 + i]))
        writes.append(pltpu.make_async_copy(out_buf.at[here], out_ref.at[here], sem.at[1, 2 + i]))
    where = pl.ds(at_ref[0], kn_buf.shape[0])
    new_reads = [pltpu.make_async_copy(src, dst, sem.at[0, 2 + pieces + i]) for i, (src, dst) in enumerate(((kn_in, kn_buf), (vn_in, vn_buf)))]
    new_writes = [pltpu.make_async_copy(src, dst.at[where], sem.at[1, 2 + pieces + i]) for i, (src, dst) in enumerate(((kn_buf, k_out), (vn_buf, v_out)))]
    for read in reads:
        read.start()

    @pl.when(is_last)
    def _():
        for read in new_reads:
            read.start()

    for read, write in zip(reads, writes):
        read.wait()
        write.start()
    for write in writes[:2]:
        write.wait()

    @pl.when(is_last)
    def _():
        for read, write in zip(new_reads, new_writes):
            read.wait()
            write.start()
        for write in new_writes:
            write.wait()

    for write in writes[2:]:
        write.wait()


def finish(n_last, write_at, out, k_shard, v_shard, k_new, v_new):
    pieces = 8
    anywhere = pl.BlockSpec(memory_space=pl.ANY)
    return pl.pallas_call(
        functools.partial(finish_kernel, n_last, pieces),
        name="finish",
        out_shape=tuple(jax.ShapeDtypeStruct(a.shape, a.dtype) for a in (out, k_shard, v_shard)),
        in_specs=[pl.BlockSpec(memory_space=pltpu.SMEM)] + [anywhere] * 5,
        out_specs=(anywhere,) * 3,
        scratch_shapes=[pltpu.VMEM(a.shape, a.dtype) for a in (out, k_shard, v_shard, k_new, v_new)] + [pltpu.SemaphoreType.DMA((2, pieces + 4))],
        compiler_params=pltpu.CompilerParams(vmem_limit_bytes=67043328),
    )(write_at.reshape(1), out, k_shard, v_shard, k_new, v_new)


def solution(mesh):
    cache_spec = P(("dp", "sp"), "tp", None)
    in_specs = (P("dp", None), P("dp"), cache_spec, cache_spec, P(None), P(None, "tp"), P(None, "tp"), P(None, "tp"), P(None), P(None), P("tp", None))
    out_specs = (P("dp", None), cache_spec, cache_spec)
    n_last = mesh.shape["sp"] - 1

    def local_step(hidden, start_pos, k_shard, v_shard, norm_gain, w_query, w_key, w_value, q_gain, k_gain, w_out):
        chunk_len, model_dim = hidden.shape
        shard_len, kv_local, head_dim = k_shard.shape
        first_pos = start_pos[0]
        cosine, sine = rope_tables(first_pos + jnp.arange(chunk_len, dtype=jnp.int32), head_dim)

        write_at = first_pos - n_last * shard_len
        k_heads, v_heads = jnp.transpose(k_shard, (1, 0, 2)), jnp.transpose(v_shard, (1, 0, 2))
        out, k_new, v_new = attend_and_combine(mesh, write_at, hidden, w_query, w_key, w_value, norm_gain, q_gain, k_gain, cosine, sine, k_heads, v_heads, w_out)
        return finish(n_last, write_at, out, k_shard, v_shard, k_new, v_new)

    return jax.shard_map(local_step, mesh=mesh, in_specs=in_specs, out_specs=out_specs, check_vma=False)
```

```python
import functools
import math

import jax
import jax.numpy as jnp
from jax import lax
from jax.experimental import pallas as pl
from jax.experimental.pallas import tpu as pltpu
from jax.sharding import PartitionSpec as P

ROPE_BASE = 1e6
NORM_EPS = 1e-6
LANES = 128
STAGES = 4
STEP_AT = (
    (5, 10, 15, 20), (6, 11, 16, 21), (9, 13, 20, 22), (11, 15, 22, 25),
    (13, 16, 24, 27), (15, 20, 26, 29), (16, 22, 28, 30), (19, 25, 30, 31),
    (22, 27, 31, 33), (23, 29, 32, 34), (24, 30, 33, 35),
)
F32 = jnp.float32
BF16 = jnp.bfloat16
MESH = pl.DeviceIdType.MESH


def rms_norm(values, gain):
    mean_sq = jnp.mean(values * values, axis=-1, keepdims=True)
    return values * lax.rsqrt(mean_sq + NORM_EPS) * gain


def rope_tables(positions, head_dim):
    half_dim = head_dim // 2
    inv_freq = ROPE_BASE ** (-2.0 * jnp.arange(half_dim, dtype=F32) / head_dim)
    angles = positions.astype(F32)[:, None] * inv_freq[None, :]
    cosine, sine = jnp.cos(angles), jnp.sin(angles)
    return cosine, sine


def merge(a, b, heads):
    d = (a.shape[1] - LANES) // heads
    sa, sb = a[:, heads * d:], b[:, heads * d:]
    top = jnp.maximum(sa, sb)
    ea, eb = jnp.exp2(sa - top), jnp.exp2(sb - top)
    lane = lax.broadcasted_iota(jnp.int32, sa.shape, 1)
    stats = jnp.where(lane < heads, top, sa * pltpu.roll(ea, heads, 1) + sb * pltpu.roll(eb, heads, 1))
    cols = [a[:, i * d:(i + 1) * d] * ea[:, i:i + 1] + b[:, i * d:(i + 1) * d] * eb[:, i:i + 1] for i in range(heads)]
    return jnp.concatenate(cols + [stats], axis=1)


def group_kernel(n_last, nx, ny, at_ref, h_hbm, wq_hbm, wk_hbm, wv_hbm, gain_ref, qg_ref, kg_ref, cos_hbm, sin_hbm, k_hbm, v_hbm, wout_hbm,
                 out_hbm, kn_hbm, vn_hbm,
                 wq, wk, wv, wout, h_buf, x_buf, cos_buf, sin_buf, k_buf, v_buf, q_buf, q_send, q_recv, s0_buf, s1_buf, p0_buf, p1_buf, bias_old, bias_new, new_f32, k_rows, v_rows,
                 msg, chip, relay_x, final_x, part, relay_y, final_y, hrow, land, outb,
                 load_sem, q_sem, table_sem, h_sem, hrow_sem, rows_sem, send_sem, recv_sem, piece_sem, share_sem, share_send, out_sem):
    stages, plane, width = chip.shape
    srows = 2 * plane
    model = wout.shape[1]
    half_model = model // 2
    xr_rows = plane // nx
    xh = xr_rows // 2
    yrows = xr_rows // ny
    sp = lax.axis_index("sp")
    y = lax.axis_index("tp")
    x, c = sp // 2, sp % 2
    oc = 1 - c
    x_r, x_l, x_o = (x + 1) % nx, (x + nx - 1) % nx, (x + 2) % nx
    y_r, y_l, y_o = (y + 1) % ny, (y + ny - 1) % ny, (y + 2) % ny
    partner = {"sp": x * 2 + oc}
    right, left = {"sp": x_r * 2 + c}, {"sp": x_l * 2 + c}
    up, down = {"tp": y_r}, {"tp": y_l}
    u = x * oc + y * c
    v = y * oc + x * c

    def axis_dev(d_first, d_second):
        return {"sp": ((x + oc * d_first + c * d_second + nx) % nx) * 2 + c, "tp": (y + c * d_first + oc * d_second + ny) % ny}

    u_r, u_l, v_r, v_l = axis_dev(1, 0), axis_dev(-1, 0), axis_dev(0, 1), axis_dev(0, -1)

    def piece_rows(du, dv):
        uu, vv = (u + du) % nx, (v + dv) % ny
        px, py = uu * oc + vv * c, vv * oc + uu * c
        return pl.multiple_of(c * plane + px * xr_rows + py * yrows, yrows)

    kv_heads, shard_len, head_dim = k_buf.shape
    own_width = wq.shape[1]
    own_heads = own_width // head_dim
    heads = 2 * own_heads
    group = heads // kv_heads
    old = shard_len - stages * srows
    pairs = heads // 2
    parts = 1 + pairs
    is_last = sp == n_last
    scale = head_dim ** -0.5 * math.log2(math.e)

    def ds(start, size):
        return pl.ds(pl.multiple_of(start, size), size)

    def q_share(b):
        return pltpu.make_async_remote_copy(
            src_ref=q_send, dst_ref=q_recv.at[b % 2], send_sem=q_sem.at[0, b], recv_sem=q_sem.at[1, b], device_id=partner, device_id_type=MESH)

    def h_load(b):
        return pltpu.make_async_copy(h_hbm.at[ds(b * srows, srows)], h_buf, h_sem.at[b])

    own_off = c * plane + x * xr_rows + y * yrows

    def hrow_load(b):
        return pltpu.make_async_copy(h_hbm.at[ds(b * srows + own_off, yrows)], hrow.at[b], hrow_sem.at[b])

    loads = [
        pltpu.make_async_copy(src, dst, load_sem.at[i])
        for i, (src, dst) in enumerate(((k_hbm, k_buf), (v_hbm, v_buf), (wout_hbm, wout), (wk_hbm, wk), (wv_hbm, wv)))
    ]
    loads.append(pltpu.make_async_copy(wq_hbm.at[:, ds(c * own_width, own_width)], wq, load_sem.at[5]))

    def table_load(b, i):
        src, dst = ((cos_hbm, cos_buf), (sin_hbm, sin_buf))[i]
        return pltpu.make_async_copy(src.at[ds(b * srows, srows)], dst.at[b % 2], table_sem.at[b, i])

    h_load(0).start()
    for i in range(2):
        table_load(0, i).start()
    loads[5].start()

    @pl.when(is_last)
    def _():
        loads[3].start()
        loads[4].start()

    loads[0].start()
    loads[1].start()
    for b in range(stages):
        hrow_load(b).start()

    barrier = pltpu.get_barrier_semaphore()
    for dev in (partner, right, left, up, down):
        pl.semaphore_signal(barrier, inc=1, device_id=dev, device_id_type=MESH)
    pl.semaphore_wait(barrier, 5)

    def copy(src, dst, ssem, rsem, dev):
        return pltpu.make_async_remote_copy(src_ref=src, dst_ref=dst, send_sem=ssem, recv_sem=rsem, device_id=dev, device_id_type=MESH)

    def m_share(b):
        return copy(msg.at[b % 2, ds(oc * plane, plane)], chip.at[b], send_sem.at[b, 0], recv_sem.at[b, 0], partner)

    def m_x(b, i):
        src, dst, dev = [
            (ds(x_o * xr_rows, xh), relay_x.at[b, 0], right),
            (ds(x_o * xr_rows + xh, xh), relay_x.at[b, 1], left),
            (ds(x_r * xr_rows + xh, xh), final_x.at[b, 0, pl.ds(xh, xh)], right),
            (ds(x_l * xr_rows, xh), final_x.at[b, 1, pl.ds(0, xh)], left),
            (ds(x_r * xr_rows, xh), final_x.at[b, 0, pl.ds(0, xh)], right),
            (ds(x_l * xr_rows + xh, xh), final_x.at[b, 1, pl.ds(xh, xh)], left),
        ][i]
        return copy(chip.at[b, src], dst, send_sem.at[b, 1 + i], recv_sem.at[b, 1 + i], dev)

    lo, hi = pl.ds(0, half_model), pl.ds(half_model, half_model)

    def m_y(b, i):
        src, dst, dev = [
            (part.at[b, ds(y_o * yrows, yrows), lo], relay_y.at[b, 0], up),
            (part.at[b, ds(y_o * yrows, yrows), hi], relay_y.at[b, 1], down),
            (part.at[b, ds(y_r * yrows, yrows), hi], final_y.at[b, 0, :, hi], up),
            (part.at[b, ds(y_l * yrows, yrows), lo], final_y.at[b, 1, :, lo], down),
            (part.at[b, ds(y_r * yrows, yrows), lo], final_y.at[b, 0, :, lo], up),
            (part.at[b, ds(y_l * yrows, yrows), hi], final_y.at[b, 1, :, hi], down),
        ][i]
        return copy(src, dst, send_sem.at[b, 7 + i], recv_sem.at[b, 7 + i], dev)

    def piece(b, du, dv, half):
        rows = pl.ds(piece_rows(du, dv), yrows)
        return land.at[b, rows] if half is None else land.at[b, rows, lo if half == 0 else hi]

    def sem_of(du, dv, half):
        return ((du % 4) * 4 + dv % 4) * 2 + (half or 0)

    def g_first(b, to, du, half):
        ref = piece(b, du, 0, half)
        s = sem_of(du - to, 0, half)
        return copy(ref, ref, send_sem.at[b, 13 + (0 if to == 1 else 1) + (2 if half is not None else 0)], piece_sem.at[b, s], u_r if to == 1 else u_l)

    def g_second(b, to, du, dv, half):
        ref = piece(b, du, dv, half)
        s = sem_of(du, dv - to, half)
        return copy(ref, ref, send_sem.at[b, 17 + (du % 4) * 4 + (0 if to == 1 else 1) + (2 if dv else 0)], piece_sem.at[b, s], v_r if to == 1 else v_l)

    def g_share(b, du, dv):
        ref = piece(b, du, dv, None)
        k = (du % 4) * 4 + dv % 4
        return copy(ref, ref, share_send.at[b, k], share_sem.at[b, k], partner)

    def wait_piece(b, du, dv, half):
        ref = piece(b, du, dv, half)
        copy(ref, ref, send_sem.at[b, 0], piece_sem.at[b, sem_of(du, dv, half)], partner).wait_recv()

    def wait_share(b, k):
        uu, vv = (x * c + y * oc + k // 4) % nx, (y * c + x * oc + k % 4) % nx
        row = oc * plane + (uu * c + vv * oc) * xr_rows + (vv * c + uu * oc) * yrows
        ref = land.at[b, pl.ds(pl.multiple_of(row, yrows), yrows)]
        copy(ref, ref, share_send.at[b, k], share_sem.at[b, k], partner).wait_recv()

    def s0(b):
        m_share(b).start()

    def s1(b):
        m_share(b).wait_recv()
        chip[b] = merge(chip[b], msg[b % 2, ds(c * plane, plane)], heads)
        for i in range(4):
            m_x(b, i).start()

    def s2(b):
        for i, dest in ((0, x_r * xr_rows), (1, x_l * xr_rows + xh)):
            m_x(b, i).wait_recv()
            rows = ds(dest, xh)
            chip[b, rows] = merge(chip[b, rows], relay_x[b, i], heads)
            m_x(b, 4 + i).start()

    def s3(b):
        @pl.when(b == 0)
        def _():
            loads[2].wait()

        for i in range(2, 6):
            m_x(b, i).wait_recv()
        total = merge(chip[b, ds(x * xr_rows, xr_rows)], final_x[b, 0], heads)
        total = merge(total, final_x[b, 1], heads)
        d = (width - LANES) // heads
        base = heads * d + heads
        att = jnp.concatenate([(total[:, i * d:(i + 1) * d] / total[:, base + i:base + i + 1]).astype(BF16) for i in range(heads)], axis=1)
        for j in range(4):
            cols = slice(j * (model // 4), (j + 1) * (model // 4))
            part[b, :, cols] = jnp.dot(att, wout[:, cols], preferred_element_type=F32)
        for i in range(4):
            m_y(b, i).start()

    def s4(b):
        for i, (dest, cols) in enumerate(((y_r, lo), (y_l, hi))):
            m_y(b, i).wait_recv()
            rows = ds(dest * yrows, yrows)
            part[b, rows, cols] = part[b, rows, cols] + relay_y[b, i]
            m_y(b, 4 + i).start()

    def s5(b):
        for i in range(2, 6):
            m_y(b, i).wait_recv()
        hrow_load(b).wait()
        total = part[b, ds(y * yrows, yrows)] + final_y[b, 0] + final_y[b, 1]
        land[b, pl.ds(piece_rows(0, 0), yrows)] = total + hrow[b].astype(F32)
        g_first(b, 1, 0, None).start()
        g_first(b, -1, 0, None).start()
        g_second(b, 1, 0, 0, None).start()
        g_second(b, -1, 0, 0, None).start()
        g_share(b, 0, 0).start()

    def arrive_second(b, du):
        wait_piece(b, du, -1, None)
        g_second(b, 1, du, -1, 0).start()
        wait_piece(b, du, 1, None)
        g_second(b, -1, du, 1, 1).start()
        g_share(b, du, -1).start()
        g_share(b, du, 1).start()

    def arrive_far(b, du):
        for half in range(2):
            wait_piece(b, du, 2, half)
        g_share(b, du, 2).start()

    def s6(b):
        wait_piece(b, -1, 0, None)
        g_first(b, 1, -1, 0).start()
        wait_piece(b, 1, 0, None)
        g_first(b, -1, 1, 1).start()
        for du in (-1, 1):
            g_second(b, 1, du, 0, None).start()
            g_second(b, -1, du, 0, None).start()
            g_share(b, du, 0).start()
        arrive_second(b, 0)

    def s7(b):
        wait_piece(b, 2, 0, 0)
        wait_piece(b, 2, 0, 1)
        g_second(b, 1, 2, 0, None).start()
        g_second(b, -1, 2, 0, None).start()
        g_share(b, 2, 0).start()
        arrive_second(b, -1)
        arrive_second(b, 1)
        arrive_far(b, 0)

    def s8(b):
        arrive_second(b, 2)
        arrive_far(b, -1)
        arrive_far(b, 1)

    def s9(b):
        arrive_far(b, 2)

    def out_copy(b, core):
        rows = ds(core * plane, plane)
        return pltpu.make_async_copy(outb.at[rows], out_hbm.at[ds(b * srows + core * plane, plane)], out_sem.at[b, 0])

    def out_copy_2(b, core):
        rows = ds(core * plane, plane)
        return pltpu.make_async_copy(outb.at[rows], out_hbm.at[ds(b * srows + core * plane, plane)], out_sem.at[b, 1])

    def write_plane(b, core):
        @pl.loop(0, plane // 16)
        def _(r):
            rows = ds(core * plane + r * 16, 16)
            outb[rows] = land[b, rows].astype(BF16)

    def s10(b):
        @pl.when(b > 0)
        def _():
            out_copy(b - 1, c).wait()
            out_copy_2(b - 1, oc).wait()

        write_plane(b, c)
        out_copy(b, c).start()
        for i in range(6):
            m_x(b, i).wait_send()
            m_y(b, i).wait_send()
        for to in (1, -1):
            g_first(b, to, 0, None).wait_send()
            g_first(b, to, -to, 0 if to == 1 else 1).wait_send()
            for du in range(4):
                g_second(b, to, du, 0, None).wait_send()
                g_second(b, to, du, -to, 0 if to == 1 else 1).wait_send()
        for du in range(4):
            for dv in range(4):
                g_share(b, du, dv).wait_send()
        for k in range(16):
            wait_share(b, k)
        write_plane(b, oc)
        out_copy_2(b, oc).start()

    lane = lax.broadcasted_iota(jnp.int32, (srows, LANES), 1)
    s_bufs, p_bufs = (s0_buf, s1_buf), (p0_buf, p1_buf)

    def kv_rows_copy(b, i):
        src, dst = ((k_rows, kn_hbm), (v_rows, vn_hbm))[i]
        return pltpu.make_async_copy(src, dst.at[ds(b * srows, srows)], rows_sem.at[b, i])

    def scores(head, slot, kb):
        q, k = q_buf[head], head // group
        nt = (((1,), (1,)), ((), ()))
        if kb is None:
            s_bufs[slot][...] = lax.dot_general(q, k_buf[k], nt, preferred_element_type=F32)
            return
        seen = old + kb * srows
        s_bufs[slot][:, :old] = lax.dot_general(q, k_buf[k, :old], nt, preferred_element_type=F32) + bias_old[...]
        if kb:
            s_bufs[slot][:, old:seen] = lax.dot_general(q, k_buf[k, old:seen], nt, preferred_element_type=F32)
        s_bufs[slot][:, seen:seen + srows] = lax.dot_general(q, k_buf[k, seen:seen + srows], nt, preferred_element_type=F32) + bias_new[...]

    def one_head(b, head, slot, kb, stats):
        keys = shard_len if kb is None else old + (kb + 1) * srows
        s = s_bufs[slot][:, :keys]
        m = jnp.max(s, axis=-1, keepdims=True)
        w = jnp.exp2((s - m) * scale)
        total = jnp.sum(w, axis=-1, keepdims=True)
        p_bufs[slot][:, :keys] = w.astype(BF16)
        num = jnp.dot(p_bufs[slot][:, :keys], v_buf[head // group, :keys], preferred_element_type=F32)
        msg[b % 2, :, pl.ds(pl.multiple_of(head * head_dim, head_dim), head_dim)] = num
        return jnp.where(lane == head, m * scale, jnp.where(lane == heads + head, total, stats))

    def each_variant(b, fn):
        @pl.when(jnp.logical_not(is_last))
        def _():
            fn(None)

        for kb in range(stages):
            @pl.when(jnp.logical_and(is_last, b == kb))
            def _():
                fn(kb)

    def project(b):
        @pl.when(b >= 2)
        def _():
            m_share(b - 2).wait_send()

        h_load(b).wait()

        @pl.loop(0, srows // 16, unroll=2)
        def _(r):
            rows = ds(r * 16, 16)
            hf = h_buf[rows].astype(F32)
            mean_sq = jnp.mean(hf * hf, axis=-1, keepdims=True)
            x_buf[rows] = (hf * lax.rsqrt(mean_sq + NORM_EPS) * gain_ref[...]).astype(BF16)

        @pl.when(b + 1 < stages)
        def _():
            h_load(b + 1).start()
            table_load(b + 1, 0).start()
            table_load(b + 1, 1).start()

        table_load(b, 0).wait()
        table_load(b, 1).wait()

        cosine, sine = cos_buf[b % 2], sin_buf[b % 2]
        cosine, sine = jnp.concatenate([cosine, cosine], axis=1), jnp.concatenate([-sine, sine], axis=1)

        def rope(one):
            return one * cosine + pltpu.roll(one, head_dim // 2, 1) * sine

        @pl.when(b == 0)
        def _():
            loads[5].wait()

        @pl.when(b > 0)
        def _():
            q_share(b - 1).wait_send()

        for pair in range(own_heads // 2):
            proj = jnp.dot(x_buf[...], wq[:, pair * 2 * head_dim:(pair + 1) * 2 * head_dim], preferred_element_type=F32)
            for j in range(2):
                one = rope(rms_norm(proj[:, j * head_dim:(j + 1) * head_dim], qg_ref[...]))
                q_send[pair * 2 + j] = one
                q_buf[c * own_heads + pair * 2 + j] = one.astype(BF16)
        q_share(b).start()

        @pl.when(b == 0)
        def _():
            loads[2].start()
            loads[0].wait()
            loads[1].wait()

        @pl.when(is_last)
        def _():
            @pl.when(b == 0)
            def _():
                loads[3].wait()
                loads[4].wait()
                key = lax.broadcasted_iota(jnp.int32, bias_old.shape, 1)
                bias_old[...] = jnp.where(key < at_ref[0], 0.0, -jnp.inf)
                row = lax.broadcasted_iota(jnp.int32, bias_new.shape, 0)
                col = lax.broadcasted_iota(jnp.int32, bias_new.shape, 1)
                bias_new[...] = jnp.where(col <= row, 0.0, -jnp.inf)

            @pl.when(b > 0)
            def _():
                kv_rows_copy(b - 1, 0).wait()
                kv_rows_copy(b - 1, 1).wait()

            new = ds(old + b * srows, srows)
            proj = jnp.dot(x_buf[...], wk[...], preferred_element_type=F32)
            for j in range(kv_heads):
                one = rope(rms_norm(proj[:, j * head_dim:(j + 1) * head_dim], kg_ref[...]))
                k_buf[j, new] = one.astype(BF16)
                new_f32[:, j, :] = one
            k_rows[...] = new_f32[...].astype(BF16)
            proj = jnp.dot(x_buf[...], wv[...], preferred_element_type=F32)
            for j in range(kv_heads):
                one = proj[:, j * head_dim:(j + 1) * head_dim]
                v_buf[j, new] = one.astype(BF16)
                new_f32[:, j, :] = one
            v_rows[...] = new_f32[...].astype(BF16)
            kv_rows_copy(b, 0).start()
            kv_rows_copy(b, 1).start()

        msg[b % 2, :, heads * head_dim:] = jnp.zeros((srows, LANES), F32)
        each_variant(b, lambda kb: scores(c * own_heads, 0, kb))

    def attend_pair(b, j):
        @pl.when(j == pairs // 2 - 1)
        def _():
            q_share(b).wait_recv()
            for i in range(own_heads):
                q_buf[oc * own_heads + i] = q_recv[b % 2, i].astype(BF16)

        head = 2 * ((j + c * (pairs // 2)) % pairs)
        after = 2 * ((jnp.minimum(j + 1, pairs - 1) + c * (pairs // 2)) % pairs)

        def run(kb):
            stats = msg[b % 2, :, heads * head_dim:]
            scores(head + 1, 1, kb)
            stats = one_head(b, head, 0, kb, stats)
            scores(after, 0, kb)
            msg[b % 2, :, heads * head_dim:] = one_head(b, head + 1, 1, kb, stats)

        each_variant(b, run)

    steps = [s0, s1, s2, s3, s4, s5, s6, s7, s8, s9, s10]

    @pl.loop(0, max(STEP_AT[-1]) + 1)
    def _(t):
        for k in reversed(range(len(steps))):
            due, passed = t == STEP_AT[k][0], 0
            for at in STEP_AT[k][1:]:
                due = jnp.logical_or(due, t == at)
                passed = passed + (t >= at).astype(jnp.int32)

            @pl.when(due)
            def _():
                steps[k](passed)

        b = t // parts

        @pl.when(jnp.logical_and(b < stages, t % parts == 0))
        def _():
            project(b)

        @pl.when(jnp.logical_and(b < stages, t % parts > 0))
        def _():
            attend_pair(b, t % parts - 1)

    @pl.when(is_last)
    def _():
        kv_rows_copy(stages - 1, 0).wait()
        kv_rows_copy(stages - 1, 1).wait()

    out_copy(stages - 1, c).wait()
    out_copy_2(stages - 1, oc).wait()
    q_share(stages - 1).wait_send()
    for b in range(stages - 2, stages):
        m_share(b).wait_send()


def attend_and_combine(mesh, write_at, hidden, w_query, w_key, w_value, norm_gain, q_gain, k_gain, cosine, sine, k_heads, v_heads, w_out):
    chunk, model = hidden.shape
    kv_heads, shard_len, head_dim = k_heads.shape
    width = w_query.shape[1] + LANES
    kv_width = w_key.shape[1]
    nx, ny = mesh.shape["sp"] // 2, mesh.shape["tp"]
    assert nx == 4 and ny == 4
    srows = chunk // STAGES
    plane = srows // 2
    xr_rows = plane // nx
    yrows = xr_rows // ny
    dma = pltpu.SemaphoreType.DMA
    anywhere = pl.BlockSpec(memory_space=pl.ANY)
    vmem = pl.BlockSpec(memory_space=pltpu.VMEM)
    new_rows = jax.ShapeDtypeStruct((chunk, kv_heads, head_dim), BF16)
    return pl.pallas_call(
        functools.partial(group_kernel, mesh.shape["sp"] - 1, nx, ny),
        name="attend_and_combine",
        out_shape=(jax.ShapeDtypeStruct((chunk, model), BF16), new_rows, new_rows),
        in_specs=[pl.BlockSpec(memory_space=pltpu.SMEM)] + [anywhere] * 4 + [vmem] * 3 + [anywhere] * 5,
        out_specs=(anywhere,) * 3,
        scratch_shapes=[
            pltpu.VMEM((model, w_query.shape[1] // 2), BF16),
            pltpu.VMEM(w_key.shape, BF16),
            pltpu.VMEM(w_value.shape, BF16),
            pltpu.VMEM(w_out.shape, BF16),
            pltpu.VMEM((srows, model), BF16),
            pltpu.VMEM((srows, model), BF16),
            pltpu.VMEM((2, srows, head_dim // 2), F32),
            pltpu.VMEM((2, srows, head_dim // 2), F32),
            pltpu.VMEM(k_heads.shape, BF16),
            pltpu.VMEM(v_heads.shape, BF16),
            pltpu.VMEM((w_query.shape[1] // head_dim, srows, head_dim), BF16),
            pltpu.VMEM((w_query.shape[1] // head_dim // 2, srows, head_dim), F32),
            pltpu.VMEM((2, w_query.shape[1] // head_dim // 2, srows, head_dim), F32),
            pltpu.VMEM((srows, shard_len), F32),
            pltpu.VMEM((srows, shard_len), F32),
            pltpu.VMEM((srows, shard_len), BF16),
            pltpu.VMEM((srows, shard_len), BF16),
            pltpu.VMEM((1, shard_len - chunk), F32),
            pltpu.VMEM((srows, srows), F32),
            pltpu.VMEM((srows, kv_heads, head_dim), F32),
            pltpu.VMEM((srows, kv_heads, head_dim), BF16),
            pltpu.VMEM((srows, kv_heads, head_dim), BF16),
            pltpu.VMEM((2, srows, width), F32),
            pltpu.VMEM((STAGES, plane, width), F32),
            pltpu.VMEM((STAGES, 2, xr_rows // 2, width), F32),
            pltpu.VMEM((STAGES, 2, xr_rows, width), F32),
            pltpu.VMEM((STAGES, xr_rows, model), F32),
            pltpu.VMEM((STAGES, 2, yrows, model // 2), F32),
            pltpu.VMEM((STAGES, 2, yrows, model), F32),
            pltpu.VMEM((STAGES, yrows, model), BF16),
            pltpu.VMEM((STAGES, srows, model), F32),
            pltpu.VMEM((srows, model), BF16),
            dma((6,)),
            dma((2, STAGES)),
            dma((STAGES, 2)),
            dma((STAGES,)),
            dma((STAGES,)),
            dma((STAGES, 2)),
            dma((STAGES, 33)),
            dma((STAGES, 13)),
            dma((STAGES, 32)),
            dma((STAGES, 16)),
            dma((STAGES, 16)),
            dma((STAGES, 2)),
        ],
        compiler_params=pltpu.CompilerParams(collective_id=0, has_side_effects=True, vmem_limit_bytes=67043328),
    )(write_at.reshape(1), hidden, w_query, w_key, w_value, norm_gain.reshape(1, model), q_gain.reshape(1, head_dim), k_gain.reshape(1, head_dim),
      cosine, sine, k_heads, v_heads, w_out)


def finish_kernel(n_last, pieces, at_ref, out_in, k_in, v_in, kn_in, vn_in, out_ref, k_out, v_out, out_buf, k_buf, v_buf, kn_buf, vn_buf, sem):
    is_last = lax.axis_index("sp") == n_last
    rows = out_in.shape[0] // pieces
    reads = [pltpu.make_async_copy(k_in, k_buf, sem.at[0, 0]), pltpu.make_async_copy(v_in, v_buf, sem.at[0, 1])]
    writes = [pltpu.make_async_copy(k_buf, k_out, sem.at[1, 0]), pltpu.make_async_copy(v_buf, v_out, sem.at[1, 1])]
    for i in range(pieces):
        here = pl.ds(i * rows, rows)
        reads.append(pltpu.make_async_copy(out_in.at[here], out_buf.at[here], sem.at[0, 2 + i]))
        writes.append(pltpu.make_async_copy(out_buf.at[here], out_ref.at[here], sem.at[1, 2 + i]))
    where = pl.ds(at_ref[0], kn_buf.shape[0])
    new_reads = [pltpu.make_async_copy(src, dst, sem.at[0, 2 + pieces + i]) for i, (src, dst) in enumerate(((kn_in, kn_buf), (vn_in, vn_buf)))]
    new_writes = [pltpu.make_async_copy(src, dst.at[where], sem.at[1, 2 + pieces + i]) for i, (src, dst) in enumerate(((kn_buf, k_out), (vn_buf, v_out)))]
    for read in reads:
        read.start()

    @pl.when(is_last)
    def _():
        for read in new_reads:
            read.start()

    for read, write in zip(reads, writes):
        read.wait()
        write.start()
    for write in writes[:2]:
        write.wait()

    @pl.when(is_last)
    def _():
        for read, write in zip(new_reads, new_writes):
            read.wait()
            write.start()
        for write in new_writes:
            write.wait()

    for write in writes[2:]:
        write.wait()


def finish(n_last, write_at, out, k_shard, v_shard, k_new, v_new):
    pieces = 8
    anywhere = pl.BlockSpec(memory_space=pl.ANY)
    return pl.pallas_call(
        functools.partial(finish_kernel, n_last, pieces),
        name="finish",
        out_shape=tuple(jax.ShapeDtypeStruct(a.shape, a.dtype) for a in (out, k_shard, v_shard)),
        in_specs=[pl.BlockSpec(memory_space=pltpu.SMEM)] + [anywhere] * 5,
        out_specs=(anywhere,) * 3,
        scratch_shapes=[pltpu.VMEM(a.shape, a.dtype) for a in (out, k_shard, v_shard, k_new, v_new)] + [pltpu.SemaphoreType.DMA((2, pieces + 4))],
        compiler_params=pltpu.CompilerParams(vmem_limit_bytes=67043328),
    )(write_at.reshape(1), out, k_shard, v_shard, k_new, v_new)


def solution(mesh):
    cache_spec = P(("dp", "sp"), "tp", None)
    in_specs = (P("dp", None), P("dp"), cache_spec, cache_spec, P(None), P(None, "tp"), P(None, "tp"), P(None, "tp"), P(None), P(None), P("tp", None))
    out_specs = (P("dp", None), cache_spec, cache_spec)
    n_last = mesh.shape["sp"] - 1

    def local_step(hidden, start_pos, k_shard, v_shard, norm_gain, w_query, w_key, w_value, q_gain, k_gain, w_out):
        chunk_len, model_dim = hidden.shape
        shard_len, kv_local, head_dim = k_shard.shape
        first_pos = start_pos[0]
        cosine, sine = rope_tables(first_pos + jnp.arange(chunk_len, dtype=jnp.int32), head_dim)

        write_at = first_pos - n_last * shard_len
        k_heads, v_heads = jnp.transpose(k_shard, (1, 0, 2)), jnp.transpose(v_shard, (1, 0, 2))
        out, k_new, v_new = attend_and_combine(mesh, write_at, hidden, w_query, w_key, w_value, norm_gain, q_gain, k_gain, cosine, sine, k_heads, v_heads, w_out)
        return finish(n_last, write_at, out, k_shard, v_shard, k_new, v_new)

    return jax.shard_map(local_step, mesh=mesh, in_specs=in_specs, out_specs=out_specs, check_vma=False)
```

```python
import functools
import math

import jax
import jax.numpy as jnp
from jax import lax
from jax.experimental import pallas as pl
from jax.experimental.pallas import tpu as pltpu
from jax.sharding import PartitionSpec as P

ROPE_BASE = 1e6
NORM_EPS = 1e-6
LANES = 128
STAGES = 4
STEP_AT = (
    (5, 10, 16, 20), (6, 11, 17, 21), (8, 13, 21, 22), (11, 15, 22, 24),
    (13, 16, 23, 25), (15, 19, 26, 27), (16, 22, 28, 29), (18, 24, 30, 31),
    (23, 25, 32, 33), (28, 31, 34, 35), (31, 34, 36, 37),
)
F32 = jnp.float32
BF16 = jnp.bfloat16
MESH = pl.DeviceIdType.MESH


def rms_norm(values, gain):
    mean_sq = jnp.mean(values * values, axis=-1, keepdims=True)
    return values * lax.rsqrt(mean_sq + NORM_EPS) * gain


def rope_tables(first_pos, chunk_len, head_dim):
    half_dim = head_dim // 2
    inv_freq = ROPE_BASE ** (-2.0 * jnp.arange(half_dim, dtype=F32) / head_dim)
    row = lax.broadcasted_iota(jnp.int32, (chunk_len // 2, head_dim), 0)
    lane = lax.broadcasted_iota(jnp.int32, (chunk_len // 2, head_dim), 1)
    positions = first_pos + row + jnp.where(lane < half_dim, 0, chunk_len // 2)
    angles = positions.astype(F32) * jnp.concatenate([inv_freq, inv_freq])[None, :]
    return jnp.cos(angles), jnp.sin(angles)


def merge(a, b, heads):
    d = (a.shape[1] - LANES) // heads
    sa, sb = a[:, heads * d:], b[:, heads * d:]
    top = jnp.maximum(sa, sb)
    ea, eb = jnp.exp2(sa - top), jnp.exp2(sb - top)
    lane = lax.broadcasted_iota(jnp.int32, sa.shape, 1)
    stats = jnp.where(lane < heads, top, sa * pltpu.roll(ea, heads, 1) + sb * pltpu.roll(eb, heads, 1))
    cols = [a[:, i * d:(i + 1) * d] * ea[:, i:i + 1] + b[:, i * d:(i + 1) * d] * eb[:, i:i + 1] for i in range(heads)]
    return jnp.concatenate(cols + [stats], axis=1)


def group_kernel(n_last, nx, ny, at_ref, h_hbm, wq_hbm, wk_hbm, wv_hbm, gain_ref, qg_ref, kg_ref, cos_hbm, sin_hbm, k_hbm, v_hbm, wout_hbm,
                 out_hbm, kn_hbm, vn_hbm,
                 wq, wk, wv, wout, h_buf, x_buf, cos_buf, sin_buf, k_buf, v_buf, q_buf, q_send, q_recv, s0_buf, s1_buf, p0_buf, p1_buf, bias_old, bias_new, new_f32, k_rows, v_rows,
                 msg, chip, relay_x, final_x, part, relay_y, final_y, hrow, land, outb,
                 load_sem, q_sem, table_sem, h_sem, hrow_sem, rows_sem, send_sem, recv_sem, piece_sem, share_sem, share_send, out_sem):
    stages, plane, width = chip.shape
    srows = 2 * plane
    model = wout.shape[1]
    half_model = model // 2
    xr_rows = plane // nx
    xh = xr_rows // 2
    yrows = xr_rows // ny
    sp = lax.axis_index("sp")
    y = lax.axis_index("tp")
    x, c = sp // 2, sp % 2
    oc = 1 - c
    x_r, x_l, x_o = (x + 1) % nx, (x + nx - 1) % nx, (x + 2) % nx
    y_r, y_l, y_o = (y + 1) % ny, (y + ny - 1) % ny, (y + 2) % ny
    partner = {"sp": x * 2 + oc}
    right, left = {"sp": x_r * 2 + c}, {"sp": x_l * 2 + c}
    up, down = {"tp": y_r}, {"tp": y_l}
    u = x * oc + y * c
    v = y * oc + x * c

    def axis_dev(d_first, d_second):
        return {"sp": ((x + oc * d_first + c * d_second + nx) % nx) * 2 + c, "tp": (y + c * d_first + oc * d_second + ny) % ny}

    u_r, u_l, v_r, v_l = axis_dev(1, 0), axis_dev(-1, 0), axis_dev(0, 1), axis_dev(0, -1)

    def piece_rows(du, dv):
        uu, vv = (u + du) % nx, (v + dv) % ny
        px, py = uu * oc + vv * c, vv * oc + uu * c
        return pl.multiple_of(c * plane + px * xr_rows + py * yrows, yrows)

    kv_heads, shard_len, head_dim = k_buf.shape
    own_width = wq.shape[1]
    own_heads = own_width // head_dim
    heads = 2 * own_heads
    group = heads // kv_heads
    old = shard_len - stages * srows
    pairs = heads // 2
    parts = 1 + pairs
    is_last = sp == n_last
    scale = head_dim ** -0.5 * math.log2(math.e)

    def ds(start, size):
        return pl.ds(pl.multiple_of(start, size), size)

    def q_share(b):
        return pltpu.make_async_remote_copy(
            src_ref=q_send, dst_ref=q_recv.at[b % 2], send_sem=q_sem.at[0, b], recv_sem=q_sem.at[1, b], device_id=partner, device_id_type=MESH)

    def h_load(b):
        return pltpu.make_async_copy(h_hbm.at[ds(b * srows, srows)], h_buf, h_sem.at[b])

    own_off = c * plane + x * xr_rows + y * yrows

    def hrow_load(b):
        return pltpu.make_async_copy(h_hbm.at[ds(b * srows + own_off, yrows)], hrow.at[b], hrow_sem.at[b])

    loads = [
        pltpu.make_async_copy(src, dst, load_sem.at[i])
        for i, (src, dst) in enumerate(((k_hbm, k_buf), (v_hbm, v_buf), (wout_hbm, wout), (wk_hbm, wk), (wv_hbm, wv)))
    ]
    loads.append(pltpu.make_async_copy(wq_hbm.at[:, ds(c * own_width, own_width)], wq, load_sem.at[5]))

    def table_load(b, i):
        src, dst = ((cos_hbm, cos_buf), (sin_hbm, sin_buf))[i]
        return pltpu.make_async_copy(src.at[ds((b % (stages // 2)) * srows, srows)], dst.at[b % 2], table_sem.at[b, i])

    h_load(0).start()
    for i in range(2):
        table_load(0, i).start()
    loads[5].start()

    @pl.when(is_last)
    def _():
        loads[3].start()
        loads[4].start()

    loads[0].start()
    loads[1].start()
    for b in range(stages):
        hrow_load(b).start()

    barrier = pltpu.get_barrier_semaphore()
    for dev in (partner, right, left, up, down):
        pl.semaphore_signal(barrier, inc=1, device_id=dev, device_id_type=MESH)

    def normalise(b):
        h_load(b).wait()

        @pl.loop(0, srows // 16, unroll=2)
        def _(r):
            rows = ds(r * 16, 16)
            hf = h_buf[rows].astype(F32)
            mean_sq = jnp.mean(hf * hf, axis=-1, keepdims=True)
            x_buf[rows] = (hf * lax.rsqrt(mean_sq + NORM_EPS) * gain_ref[...]).astype(BF16)

    normalise(0)
    pl.semaphore_wait(barrier, 5)

    def copy(src, dst, ssem, rsem, dev):
        return pltpu.make_async_remote_copy(src_ref=src, dst_ref=dst, send_sem=ssem, recv_sem=rsem, device_id=dev, device_id_type=MESH)

    def m_share(b):
        return copy(msg.at[b % 2, ds(oc * plane, plane)], chip.at[b], send_sem.at[b, 0], recv_sem.at[b, 0], partner)

    def m_x(b, i):
        src, dst, dev = [
            (ds(x_o * xr_rows, xh), relay_x.at[b, 0], right),
            (ds(x_o * xr_rows + xh, xh), relay_x.at[b, 1], left),
            (ds(x_r * xr_rows + xh, xh), final_x.at[b, 0, pl.ds(xh, xh)], right),
            (ds(x_l * xr_rows, xh), final_x.at[b, 1, pl.ds(0, xh)], left),
            (ds(x_r * xr_rows, xh), final_x.at[b, 0, pl.ds(0, xh)], right),
            (ds(x_l * xr_rows + xh, xh), final_x.at[b, 1, pl.ds(xh, xh)], left),
        ][i]
        return copy(chip.at[b, src], dst, send_sem.at[b, 1 + i], recv_sem.at[b, 1 + i], dev)

    lo, hi = pl.ds(0, half_model), pl.ds(half_model, half_model)

    def m_y(b, i):
        src, dst, dev = [
            (part.at[b, ds(y_o * yrows, yrows), lo], relay_y.at[b, 0], up),
            (part.at[b, ds(y_o * yrows, yrows), hi], relay_y.at[b, 1], down),
            (part.at[b, ds(y_r * yrows, yrows), hi], final_y.at[b, 0, :, hi], up),
            (part.at[b, ds(y_l * yrows, yrows), lo], final_y.at[b, 1, :, lo], down),
            (part.at[b, ds(y_r * yrows, yrows), lo], final_y.at[b, 0, :, lo], up),
            (part.at[b, ds(y_l * yrows, yrows), hi], final_y.at[b, 1, :, hi], down),
        ][i]
        return copy(src, dst, send_sem.at[b, 7 + i], recv_sem.at[b, 7 + i], dev)

    def piece(b, du, dv, half):
        rows = pl.ds(piece_rows(du, dv), yrows)
        return land.at[b, rows] if half is None else land.at[b, rows, lo if half == 0 else hi]

    def sem_of(du, dv, half):
        return ((du % 4) * 4 + dv % 4) * 2 + (half or 0)

    def g_first(b, to, du, half):
        ref = piece(b, du, 0, half)
        s = sem_of(du - to, 0, half)
        return copy(ref, ref, send_sem.at[b, 13 + (0 if to == 1 else 1) + (2 if half is not None else 0)], piece_sem.at[b, s], u_r if to == 1 else u_l)

    def g_second(b, to, du, dv, half):
        ref = piece(b, du, dv, half)
        s = sem_of(du, dv - to, half)
        return copy(ref, ref, send_sem.at[b, 17 + (du % 4) * 4 + (0 if to == 1 else 1) + (2 if dv else 0)], piece_sem.at[b, s], v_r if to == 1 else v_l)

    def g_share(b, du, dv):
        ref = piece(b, du, dv, None)
        k = (du % 4) * 4 + dv % 4
        return copy(ref, ref, share_send.at[b, k], share_sem.at[b, k], partner)

    def wait_piece(b, du, dv, half):
        ref = piece(b, du, dv, half)
        copy(ref, ref, send_sem.at[b, 0], piece_sem.at[b, sem_of(du, dv, half)], partner).wait_recv()

    def wait_share(b, k):
        uu, vv = (x * c + y * oc + k // 4) % nx, (y * c + x * oc + k % 4) % nx
        row = oc * plane + (uu * c + vv * oc) * xr_rows + (vv * c + uu * oc) * yrows
        ref = land.at[b, pl.ds(pl.multiple_of(row, yrows), yrows)]
        copy(ref, ref, share_send.at[b, k], share_sem.at[b, k], partner).wait_recv()

    def s0(b):
        m_share(b).start()

    def s1(b):
        m_share(b).wait_recv()
        chip[b] = merge(chip[b], msg[b % 2, ds(c * plane, plane)], heads)
        for i in range(4):
            m_x(b, i).start()

    def s2(b):
        for i, dest in ((0, x_r * xr_rows), (1, x_l * xr_rows + xh)):
            m_x(b, i).wait_recv()
            rows = ds(dest, xh)
            chip[b, rows] = merge(chip[b, rows], relay_x[b, i], heads)
            m_x(b, 4 + i).start()

    def s3(b):
        @pl.when(b == 0)
        def _():
            loads[2].wait()

        for i in range(2, 6):
            m_x(b, i).wait_recv()
        total = merge(chip[b, ds(x * xr_rows, xr_rows)], final_x[b, 0], heads)
        total = merge(total, final_x[b, 1], heads)
        d = (width - LANES) // heads
        base = heads * d + heads
        att = jnp.concatenate([(total[:, i * d:(i + 1) * d] / total[:, base + i:base + i + 1]).astype(BF16) for i in range(heads)], axis=1)
        for j in range(4):
            cols = slice(j * (model // 4), (j + 1) * (model // 4))
            part[b, :, cols] = jnp.dot(att, wout[:, cols], preferred_element_type=F32)
        for i in range(4):
            m_y(b, i).start()

    def s4(b):
        for i, (dest, cols) in enumerate(((y_r, lo), (y_l, hi))):
            m_y(b, i).wait_recv()
            rows = ds(dest * yrows, yrows)
            part[b, rows, cols] = part[b, rows, cols] + relay_y[b, i]
            m_y(b, 4 + i).start()

    def s5(b):
        for i in range(2, 6):
            m_y(b, i).wait_recv()
        hrow_load(b).wait()
        total = part[b, ds(y * yrows, yrows)] + final_y[b, 0] + final_y[b, 1]
        land[b, pl.ds(piece_rows(0, 0), yrows)] = total + hrow[b].astype(F32)
        g_first(b, 1, 0, None).start()
        g_first(b, -1, 0, None).start()
        g_second(b, 1, 0, 0, None).start()
        g_second(b, -1, 0, 0, None).start()
        g_share(b, 0, 0).start()

    def arrive_second(b, du):
        wait_piece(b, du, -1, None)
        g_second(b, 1, du, -1, 0).start()
        wait_piece(b, du, 1, None)
        g_second(b, -1, du, 1, 1).start()
        g_share(b, du, -1).start()
        g_share(b, du, 1).start()

    def arrive_far(b, du):
        for half in range(2):
            wait_piece(b, du, 2, half)
        g_share(b, du, 2).start()

    def s6(b):
        wait_piece(b, -1, 0, None)
        g_first(b, 1, -1, 0).start()
        wait_piece(b, 1, 0, None)
        g_first(b, -1, 1, 1).start()
        for du in (-1, 1):
            g_second(b, 1, du, 0, None).start()
            g_second(b, -1, du, 0, None).start()
            g_share(b, du, 0).start()
        arrive_second(b, 0)

    def s7(b):
        wait_piece(b, 2, 0, 0)
        wait_piece(b, 2, 0, 1)
        g_second(b, 1, 2, 0, None).start()
        g_second(b, -1, 2, 0, None).start()
        g_share(b, 2, 0).start()
        arrive_second(b, -1)
        arrive_second(b, 1)
        arrive_far(b, 0)

    def s8(b):
        arrive_second(b, 2)
        arrive_far(b, -1)
        arrive_far(b, 1)

    def s9(b):
        arrive_far(b, 2)

    def out_copy(b, core):
        rows = ds(core * plane, plane)
        return pltpu.make_async_copy(outb.at[rows], out_hbm.at[ds(b * srows + core * plane, plane)], out_sem.at[b, 0])

    def out_copy_2(b, core):
        rows = ds(core * plane, plane)
        return pltpu.make_async_copy(outb.at[rows], out_hbm.at[ds(b * srows + core * plane, plane)], out_sem.at[b, 1])

    def write_plane(b, core):
        @pl.loop(0, plane // 16)
        def _(r):
            rows = ds(core * plane + r * 16, 16)
            outb[rows] = land[b, rows].astype(BF16)

    def s10(b):
        @pl.when(b > 0)
        def _():
            out_copy(b - 1, c).wait()
            out_copy_2(b - 1, oc).wait()

        write_plane(b, c)
        out_copy(b, c).start()
        for i in range(6):
            m_x(b, i).wait_send()
            m_y(b, i).wait_send()
        for to in (1, -1):
            g_first(b, to, 0, None).wait_send()
            g_first(b, to, -to, 0 if to == 1 else 1).wait_send()
            for du in range(4):
                g_second(b, to, du, 0, None).wait_send()
                g_second(b, to, du, -to, 0 if to == 1 else 1).wait_send()
        for du in range(4):
            for dv in range(4):
                g_share(b, du, dv).wait_send()
        for k in range(16):
            wait_share(b, k)
        write_plane(b, oc)
        out_copy_2(b, oc).start()

    lane = lax.broadcasted_iota(jnp.int32, (srows, LANES), 1)
    s_bufs, p_bufs = (s0_buf, s1_buf), (p0_buf, p1_buf)

    def kv_rows_copy(b, i):
        src, dst = ((k_rows, kn_hbm), (v_rows, vn_hbm))[i]
        return pltpu.make_async_copy(src, dst.at[ds(b * srows, srows)], rows_sem.at[b, i])

    def scores(head, slot, kb):
        q, k = q_buf[head], head // group
        nt = (((1,), (1,)), ((), ()))
        if kb is None:
            s_bufs[slot][...] = lax.dot_general(q, k_buf[k], nt, preferred_element_type=F32)
            return
        seen = old + kb * srows
        s_bufs[slot][:, :old] = lax.dot_general(q, k_buf[k, :old], nt, preferred_element_type=F32) + bias_old[...]
        if kb:
            s_bufs[slot][:, old:seen] = lax.dot_general(q, k_buf[k, old:seen], nt, preferred_element_type=F32)
        s_bufs[slot][:, seen:seen + srows] = lax.dot_general(q, k_buf[k, seen:seen + srows], nt, preferred_element_type=F32) + bias_new[...]

    def one_head(b, head, slot, kb, stats):
        keys = shard_len if kb is None else old + (kb + 1) * srows
        s = s_bufs[slot][:, :keys]
        m = jnp.max(s, axis=-1, keepdims=True)
        w = jnp.exp2((s - m) * scale)
        total = jnp.sum(w, axis=-1, keepdims=True)
        p_bufs[slot][:, :keys] = w.astype(BF16)
        num = jnp.dot(p_bufs[slot][:, :keys], v_buf[head // group, :keys], preferred_element_type=F32)
        msg[b % 2, :, pl.ds(pl.multiple_of(head * head_dim, head_dim), head_dim)] = num
        return jnp.where(lane == head, m * scale, jnp.where(lane == heads + head, total, stats))

    def each_variant(b, fn):
        @pl.when(jnp.logical_not(is_last))
        def _():
            fn(None)

        for kb in range(stages):
            @pl.when(jnp.logical_and(is_last, b == kb))
            def _():
                fn(kb)

    def project(b):
        @pl.when(b >= 2)
        def _():
            m_share(b - 2).wait_send()

        @pl.when(b > 0)
        def _():
            normalise(b)

        @pl.when(b + 1 < stages)
        def _():
            h_load(b + 1).start()
            table_load(b + 1, 0).start()
            table_load(b + 1, 1).start()

        table_load(b, 0).wait()
        table_load(b, 1).wait()

        low = lane < head_dim // 2
        here = low == (b < stages // 2)
        cosine, sine = (jnp.where(here, table[b % 2], pltpu.roll(table[b % 2], head_dim // 2, 1)) for table in (cos_buf, sin_buf))
        sine = jnp.where(low, -sine, sine)

        def rope(one):
            return one * cosine + pltpu.roll(one, head_dim // 2, 1) * sine

        @pl.when(b == 0)
        def _():
            loads[5].wait()

        @pl.when(b > 0)
        def _():
            q_share(b - 1).wait_send()

        for pair in range(own_heads // 2):
            proj = jnp.dot(x_buf[...], wq[:, pair * 2 * head_dim:(pair + 1) * 2 * head_dim], preferred_element_type=F32)
            for j in range(2):
                one = rope(rms_norm(proj[:, j * head_dim:(j + 1) * head_dim], qg_ref[...]))
                q_send[pair * 2 + j] = one
                q_buf[c * own_heads + pair * 2 + j] = one.astype(BF16)
        q_share(b).start()

        @pl.when(b == 0)
        def _():
            loads[2].start()
            loads[0].wait()
            loads[1].wait()

        @pl.when(is_last)
        def _():
            @pl.when(b == 0)
            def _():
                loads[3].wait()
                loads[4].wait()
                key = lax.broadcasted_iota(jnp.int32, bias_old.shape, 1)
                bias_old[...] = jnp.where(key < at_ref[0], 0.0, -jnp.inf)
                row = lax.broadcasted_iota(jnp.int32, bias_new.shape, 0)
                col = lax.broadcasted_iota(jnp.int32, bias_new.shape, 1)
                bias_new[...] = jnp.where(col <= row, 0.0, -jnp.inf)

            @pl.when(b > 0)
            def _():
                kv_rows_copy(b - 1, 0).wait()
                kv_rows_copy(b - 1, 1).wait()

            new = ds(old + b * srows, srows)
            proj = jnp.dot(x_buf[...], wk[...], preferred_element_type=F32)
            for j in range(kv_heads):
                one = rope(rms_norm(proj[:, j * head_dim:(j + 1) * head_dim], kg_ref[...]))
                k_buf[j, new] = one.astype(BF16)
                new_f32[:, j, :] = one
            k_rows[...] = new_f32[...].astype(BF16)
            proj = jnp.dot(x_buf[...], wv[...], preferred_element_type=F32)
            for j in range(kv_heads):
                one = proj[:, j * head_dim:(j + 1) * head_dim]
                v_buf[j, new] = one.astype(BF16)
                new_f32[:, j, :] = one
            v_rows[...] = new_f32[...].astype(BF16)
            kv_rows_copy(b, 0).start()
            kv_rows_copy(b, 1).start()

        msg[b % 2, :, heads * head_dim:] = jnp.zeros((srows, LANES), F32)
        each_variant(b, lambda kb: scores(c * own_heads, 0, kb))

    def attend_pair(b, j):
        @pl.when(j == pairs // 2 - 1)
        def _():
            q_share(b).wait_recv()
            for i in range(own_heads):
                q_buf[oc * own_heads + i] = q_recv[b % 2, i].astype(BF16)

        head = 2 * ((j + c * (pairs // 2)) % pairs)
        after = 2 * ((jnp.minimum(j + 1, pairs - 1) + c * (pairs // 2)) % pairs)

        def run(kb):
            stats = msg[b % 2, :, heads * head_dim:]
            scores(head + 1, 1, kb)
            stats = one_head(b, head, 0, kb, stats)
            scores(after, 0, kb)
            msg[b % 2, :, heads * head_dim:] = one_head(b, head + 1, 1, kb, stats)

        each_variant(b, run)

    steps = [s0, s1, s2, s3, s4, s5, s6, s7, s8, s9, s10]

    @pl.loop(0, max(STEP_AT[-1]) + 1)
    def _(t):
        for k in reversed(range(len(steps))):
            due, passed = t == STEP_AT[k][0], 0
            for at in STEP_AT[k][1:]:
                due = jnp.logical_or(due, t == at)
                passed = passed + (t >= at).astype(jnp.int32)

            @pl.when(due)
            def _():
                steps[k](passed)

        b = t // parts

        @pl.when(jnp.logical_and(b < stages, t % parts == 0))
        def _():
            project(b)

        @pl.when(jnp.logical_and(b < stages, t % parts > 0))
        def _():
            attend_pair(b, t % parts - 1)

    @pl.when(is_last)
    def _():
        kv_rows_copy(stages - 1, 0).wait()
        kv_rows_copy(stages - 1, 1).wait()

    out_copy(stages - 1, c).wait()
    out_copy_2(stages - 1, oc).wait()
    q_share(stages - 1).wait_send()
    for b in range(stages - 2, stages):
        m_share(b).wait_send()


def attend_and_combine(mesh, write_at, hidden, w_query, w_key, w_value, norm_gain, q_gain, k_gain, cosine, sine, k_heads, v_heads, w_out):
    chunk, model = hidden.shape
    kv_heads, shard_len, head_dim = k_heads.shape
    width = w_query.shape[1] + LANES
    kv_width = w_key.shape[1]
    nx, ny = mesh.shape["sp"] // 2, mesh.shape["tp"]
    assert nx == 4 and ny == 4
    srows = chunk // STAGES
    plane = srows // 2
    xr_rows = plane // nx
    yrows = xr_rows // ny
    dma = pltpu.SemaphoreType.DMA
    anywhere = pl.BlockSpec(memory_space=pl.ANY)
    vmem = pl.BlockSpec(memory_space=pltpu.VMEM)
    new_rows = jax.ShapeDtypeStruct((chunk, kv_heads, head_dim), BF16)
    return pl.pallas_call(
        functools.partial(group_kernel, mesh.shape["sp"] - 1, nx, ny),
        name="attend_and_combine",
        out_shape=(jax.ShapeDtypeStruct((chunk, model), BF16), new_rows, new_rows),
        in_specs=[pl.BlockSpec(memory_space=pltpu.SMEM)] + [anywhere] * 4 + [vmem] * 3 + [anywhere] * 5,
        out_specs=(anywhere,) * 3,
        scratch_shapes=[
            pltpu.VMEM((model, w_query.shape[1] // 2), BF16),
            pltpu.VMEM(w_key.shape, BF16),
            pltpu.VMEM(w_value.shape, BF16),
            pltpu.VMEM(w_out.shape, BF16),
            pltpu.VMEM((srows, model), BF16),
            pltpu.VMEM((srows, model), BF16),
            pltpu.VMEM((2, srows, head_dim), F32),
            pltpu.VMEM((2, srows, head_dim), F32),
            pltpu.VMEM(k_heads.shape, BF16),
            pltpu.VMEM(v_heads.shape, BF16),
            pltpu.VMEM((w_query.shape[1] // head_dim, srows, head_dim), BF16),
            pltpu.VMEM((w_query.shape[1] // head_dim // 2, srows, head_dim), F32),
            pltpu.VMEM((2, w_query.shape[1] // head_dim // 2, srows, head_dim), F32),
            pltpu.VMEM((srows, shard_len), F32),
            pltpu.VMEM((srows, shard_len), F32),
            pltpu.VMEM((srows, shard_len), BF16),
            pltpu.VMEM((srows, shard_len), BF16),
            pltpu.VMEM((1, shard_len - chunk), F32),
            pltpu.VMEM((srows, srows), F32),
            pltpu.VMEM((srows, kv_heads, head_dim), F32),
            pltpu.VMEM((srows, kv_heads, head_dim), BF16),
            pltpu.VMEM((srows, kv_heads, head_dim), BF16),
            pltpu.VMEM((2, srows, width), F32),
            pltpu.VMEM((STAGES, plane, width), F32),
            pltpu.VMEM((STAGES, 2, xr_rows // 2, width), F32),
            pltpu.VMEM((STAGES, 2, xr_rows, width), F32),
            pltpu.VMEM((STAGES, xr_rows, model), F32),
            pltpu.VMEM((STAGES, 2, yrows, model // 2), F32),
            pltpu.VMEM((STAGES, 2, yrows, model), F32),
            pltpu.VMEM((STAGES, yrows, model), BF16),
            pltpu.VMEM((STAGES, srows, model), F32),
            pltpu.VMEM((srows, model), BF16),
            dma((6,)),
            dma((2, STAGES)),
            dma((STAGES, 2)),
            dma((STAGES,)),
            dma((STAGES,)),
            dma((STAGES, 2)),
            dma((STAGES, 33)),
            dma((STAGES, 13)),
            dma((STAGES, 32)),
            dma((STAGES, 16)),
            dma((STAGES, 16)),
            dma((STAGES, 2)),
        ],
        compiler_params=pltpu.CompilerParams(collective_id=0, has_side_effects=True, vmem_limit_bytes=67043328),
    )(write_at.reshape(1), hidden, w_query, w_key, w_value, norm_gain.reshape(1, model), q_gain.reshape(1, head_dim), k_gain.reshape(1, head_dim),
      cosine, sine, k_heads, v_heads, w_out)


def finish_kernel(n_last, pieces, at_ref, out_in, k_in, v_in, kn_in, vn_in, out_ref, k_out, v_out, out_buf, k_buf, v_buf, kn_buf, vn_buf, sem):
    is_last = lax.axis_index("sp") == n_last
    rows = out_in.shape[0] // pieces
    reads = [pltpu.make_async_copy(k_in, k_buf, sem.at[0, 0]), pltpu.make_async_copy(v_in, v_buf, sem.at[0, 1])]
    writes = [pltpu.make_async_copy(k_buf, k_out, sem.at[1, 0]), pltpu.make_async_copy(v_buf, v_out, sem.at[1, 1])]
    for i in range(pieces):
        here = pl.ds(i * rows, rows)
        reads.append(pltpu.make_async_copy(out_in.at[here], out_buf.at[here], sem.at[0, 2 + i]))
        writes.append(pltpu.make_async_copy(out_buf.at[here], out_ref.at[here], sem.at[1, 2 + i]))
    where = pl.ds(at_ref[0], kn_buf.shape[0])
    new_reads = [pltpu.make_async_copy(src, dst, sem.at[0, 2 + pieces + i]) for i, (src, dst) in enumerate(((kn_in, kn_buf), (vn_in, vn_buf)))]
    new_writes = [pltpu.make_async_copy(src, dst.at[where], sem.at[1, 2 + pieces + i]) for i, (src, dst) in enumerate(((kn_buf, k_out), (vn_buf, v_out)))]
    for read in reads:
        read.start()

    @pl.when(is_last)
    def _():
        for read in new_reads:
            read.start()

    for read, write in zip(reads, writes):
        read.wait()
        write.start()
    for write in writes[:2]:
        write.wait()

    @pl.when(is_last)
    def _():
        for read, write in zip(new_reads, new_writes):
            read.wait()
            write.start()
        for write in new_writes:
            write.wait()

    for write in writes[2:]:
        write.wait()


def finish(n_last, write_at, out, k_shard, v_shard, k_new, v_new):
    pieces = 16
    anywhere = pl.BlockSpec(memory_space=pl.ANY)
    return pl.pallas_call(
        functools.partial(finish_kernel, n_last, pieces),
        name="finish",
        out_shape=tuple(jax.ShapeDtypeStruct(a.shape, a.dtype) for a in (out, k_shard, v_shard)),
        in_specs=[pl.BlockSpec(memory_space=pltpu.SMEM)] + [anywhere] * 5,
        out_specs=(anywhere,) * 3,
        scratch_shapes=[pltpu.VMEM(a.shape, a.dtype) for a in (out, k_shard, v_shard, k_new, v_new)] + [pltpu.SemaphoreType.DMA((2, pieces + 4))],
        compiler_params=pltpu.CompilerParams(vmem_limit_bytes=67043328),
    )(write_at.reshape(1), out, k_shard, v_shard, k_new, v_new)


def solution(mesh):
    cache_spec = P(("dp", "sp"), "tp", None)
    in_specs = (P("dp", None), P("dp"), cache_spec, cache_spec, P(None), P(None, "tp"), P(None, "tp"), P(None, "tp"), P(None), P(None), P("tp", None))
    out_specs = (P("dp", None), cache_spec, cache_spec)
    n_last = mesh.shape["sp"] - 1

    def local_step(hidden, start_pos, k_shard, v_shard, norm_gain, w_query, w_key, w_value, q_gain, k_gain, w_out):
        chunk_len, model_dim = hidden.shape
        shard_len, kv_local, head_dim = k_shard.shape
        first_pos = start_pos[0]
        cosine, sine = rope_tables(first_pos, chunk_len, head_dim)

        write_at = first_pos - n_last * shard_len
        k_heads, v_heads = jnp.transpose(k_shard, (1, 0, 2)), jnp.transpose(v_shard, (1, 0, 2))
        out, k_new, v_new = attend_and_combine(mesh, write_at, hidden, w_query, w_key, w_value, norm_gain, q_gain, k_gain, cosine, sine, k_heads, v_heads, w_out)
        return finish(n_last, write_at, out, k_shard, v_shard, k_new, v_new)

    return jax.shard_map(local_step, mesh=mesh, in_specs=in_specs, out_specs=out_specs, check_vma=False)
```
